256 devices in a mesh: tm: 32 (over z, y), space: 8 (over x, core).
Axes of the slice: x: 4, y: 4, z: 8, core: 2. Of those that a mesh axis runs over, the one named last changes fastest.
Arguments:
- start_values: float32 [32, 2, 1024, 1024], P('tm', None, 'space'), may hold values from -6 to 6
- node_values: float32 [32, 2, 2, 1024, 1024], P('tm', None, None, 'space'), may hold values from -6 to 6
Outputs:
- next_start: float32 [32, 2, 1024, 1024], P('tm', None, 'space')
- next_nodes: float32 [32, 2, 2, 1024, 1024], P('tm', None, None, 'space')
The draws below stay inside these ranges and needn't reach their ends.
All inputs are finite; a program needn't handle non-finite values.
Results may differ from the reference program's by a relative error of at most 0.00002.
Values sent between devices are 32-bit elements; how exact they have to be, the bound alone decides.
A program may use at most 64 MiB of HBM per device.

```python
import jax
import jax.numpy as jnp
from jax import lax

KX = 1024
KY = 1024
CX = 256
NT = 32


def block_scale(stream_key, dims, shards, low, largest):
    loudness, own = 1.0, jax.random.fold_in(stream_key, 6)
    for dim, shards_of in shards:
        heights = jnp.exp(jax.random.uniform(jax.random.fold_in(own, dim), (shards_of,), jnp.float32, low / len(shards), largest / len(shards)))
        loudness = loudness * jnp.repeat(heights, dims[dim] // shards_of).reshape([-1 if axis == dim else 1 for axis in range(len(dims))])
    return loudness


def scatter_about(key, dims, width, reach, pieces=(), held_as=jnp.bfloat16):
    factor_of = block_scale(key, dims, pieces, -0.22, 0.18) if pieces else 1.0
    values = jax.random.normal(key, dims, jnp.float32) * width * factor_of
    return jnp.minimum(jnp.maximum(values, -reach), reach).astype(held_as)


def setup_inputs(seed: int = 0) -> dict:
    key_list = jax.random.split(jax.random.key(seed), 3)
    start_values = scatter_about(key_list[0], (NT, 2, KX, KY), 1.0, 6.0, ((0, 32), (2, 8)), jnp.float32)
    node_values = scatter_about(key_list[1], (NT, 2, 2, KX, KY), 1.0, 6.0, ((0, 32), (3, 8)), jnp.float32)
    return dict(start_values=start_values, node_values=node_values)


diffusion = 1.5
drift = 0.8
shear = 0.6
first_weights = (5.0 / 24.0, 1.0 / 3.0, -1.0 / 24.0)
second_weights = (-1.0 / 24.0, 1.0 / 3.0, 5.0 / 24.0)
whole_weights = (1.0 / 6.0, 2.0 / 3.0, 1.0 / 6.0)


def spectrum(row_index, column_index):
    along = (row_index.astype(jnp.float32) - KX // 2) / (KX // 2)
    across = (column_index.astype(jnp.float32) - KY // 2) / (KY // 2)
    real_rate = -diffusion * (along[:, None] * along[:, None] + across[None, :] * across[None, :])
    imag_rate = -drift * across[None, :] + 0.0 * along[:, None]
    return real_rate, imag_rate, across


def multiply(real_rate, imag_rate, field):
    return jnp.stack([real_rate * field[..., 0, :, :] - imag_rate * field[..., 1, :, :],
                      real_rate * field[..., 1, :, :] + imag_rate * field[..., 0, :, :]], axis=-3)


def divide(real_part, imag_part, field):
    modulus = real_part * real_part + imag_part * imag_part
    return jnp.stack([(field[..., 0, :, :] * real_part + field[..., 1, :, :] * imag_part) / modulus,
                      (field[..., 1, :, :] * real_part - field[..., 0, :, :] * imag_part) / modulus], axis=-3)


def coupling_of(padded, across):
    sums = padded[..., 2:, :] + padded[..., :-2, :]
    factor = shear * across
    return jnp.stack([factor * sums[..., 1, :, :], -factor * sums[..., 0, :, :]], axis=-3)


def explicit(field, across):
    widths = [(0, 0)] * (field.ndim - 2) + [(1, 1), (0, 0)]
    return coupling_of(jnp.pad(field, widths), across)


def fine_section(begin_value, old_nodes):
    real_rate, imag_rate, across = spectrum(jnp.arange(KX), jnp.arange(KY))
    stacked = jnp.stack([begin_value, old_nodes[0], old_nodes[1]])
    old_coupling = explicit(stacked, across)
    old_slopes = multiply(real_rate, imag_rate, stacked) + old_coupling
    sum_one = first_weights[0] * old_slopes[0] + first_weights[1] * old_slopes[1] + first_weights[2] * old_slopes[2]
    sum_two = second_weights[0] * old_slopes[0] + second_weights[1] * old_slopes[1] + second_weights[2] * old_slopes[2]
    half_real = 1.0 - 0.5 * real_rate
    half_imag = -0.5 * imag_rate
    node_one = divide(half_real, half_imag, begin_value - 0.5 * multiply(real_rate, imag_rate, old_nodes[0]) + sum_one)
    one_coupling = explicit(node_one[None], across)[0]
    node_two = divide(half_real, half_imag, node_one + 0.5 * (one_coupling - old_coupling[1])
                      - 0.5 * multiply(real_rate, imag_rate, old_nodes[1]) + sum_two)
    two_coupling = explicit(node_two[None], across)[0]
    integral = (whole_weights[0] * old_slopes[0]
                + whole_weights[1] * (multiply(real_rate, imag_rate, node_one) + one_coupling)
                + whole_weights[2] * (multiply(real_rate, imag_rate, node_two) + two_coupling))
    low_row = KX // 2 - CX // 2
    low_column = KY // 2 - CX // 2
    coarse_real = real_rate[low_row:low_row + CX, low_column:low_column + CX]
    coarse_imag = imag_rate[low_row:low_row + CX, low_column:low_column + CX]
    begin_coarse = begin_value[:, low_row:low_row + CX, low_column:low_column + CX]
    end_coarse = node_two[:, low_row:low_row + CX, low_column:low_column + CX]
    tau = integral[:, low_row:low_row + CX, low_column:low_column + CX] - 0.5 * multiply(coarse_real, coarse_imag, begin_coarse + end_coarse)
    offset = 0.5 * multiply(coarse_real, coarse_imag, begin_coarse - end_coarse) + tau
    return node_one, node_two, begin_coarse, end_coarse, offset


def reference(start_values, node_values):
    node_one, node_two, begin_coarse, end_coarse, offset = lax.map(
        lambda paired: fine_section(paired[0], paired[1]), (start_values, node_values))
    real_rate, imag_rate, across = spectrum(jnp.arange(KX), jnp.arange(KY))
    low_row = KX // 2 - CX // 2
    low_column = KY // 2 - CX // 2
    coarse_real = real_rate[low_row:low_row + CX, low_column:low_column + CX]
    coarse_imag = imag_rate[low_row:low_row + CX, low_column:low_column + CX]
    step_real = 1.0 - coarse_real
    step_imag = -coarse_imag
    coarse_starts = [begin_coarse[0]]
    for slice_index in range(1, NT):
        coarse_starts.append(divide(step_real, step_imag, coarse_starts[-1] + offset[slice_index - 1]))
    begin_new = jnp.stack(coarse_starts)
    end_new = divide(step_real, step_imag, begin_new + offset)
    delta_begin = begin_new - begin_coarse
    delta_end = end_new - end_coarse
    widths = ((0, 0), (0, 0), (low_row, KX - low_row - CX), (low_column, KY - low_column - CX))
    fixed_one = node_one + jnp.pad(0.5 * (delta_begin + delta_end), widths)
    fixed_two = node_two + jnp.pad(delta_end, widths)
    next_start = jnp.concatenate([start_values[:1], fixed_two[:-1]], axis=0)
    next_nodes = jnp.stack([fixed_one, fixed_two], axis=1)
    return (next_start, next_nodes)
```

```python
import functools

import jax
import jax.numpy as jnp
from jax import lax
from jax.experimental import pallas as pl
from jax.experimental.pallas import tpu as pltpu
from jax.sharding import PartitionSpec as P

MESH = pl.DeviceIdType.MESH
F32 = jnp.float32
KX = 1024
KY = 1024
CX = 256
LANES = 128
ROWS = 128
TILES = KY // LANES
FIRST_COARSE_TILE = (KY // 2 - CX // 2) // LANES
COARSE_TILES = CX // LANES
FIRST_COARSE_RANK = (KX // 2 - CX // 2) // ROWS
COARSE_RANKS = CX // ROWS
FINE_TILES = [t for t in range(TILES) if not FIRST_COARSE_TILE <= t < FIRST_COARSE_TILE + COARSE_TILES]

diffusion = 1.5
drift = 0.8
shear = 0.6


def columns(tile):
    return pl.ds(pl.multiple_of(tile * LANES, LANES), LANES)


def rate_of(first_row, first_column, rows):
    row = (first_row + lax.broadcasted_iota(jnp.int32, (rows, LANES), 0)).astype(F32)
    column = (first_column + lax.broadcasted_iota(jnp.int32, (rows, LANES), 1)).astype(F32)
    along = (row - KX // 2) / (KX // 2)
    across = (column - KY // 2) / (KY // 2)
    return -diffusion * (along * along + across * across), -drift * across, shear * across


def times(ar, ai, br, bi):
    return ar * br - ai * bi, ar * bi + ai * br


def inverse(real_part, imag_part):
    scale = 1.0 / (real_part * real_part + imag_part * imag_part)
    return real_part * scale, -imag_part * scale


def kernel(tm_size, space_size, start_hbm, nodes_hbm, next_out, nodes_out, fields, mixed, staged, node_one_buf, whole, offset,
           gathered, scanned, begins, load_sem, halo_send, halo_recv, bulk_send, bulk_recv, gather_send, gather_recv,
           scatter_send, scatter_recv):
    slot = lax.axis_index("tm")
    rank = lax.axis_index("space")
    coarse = (rank >= FIRST_COARSE_RANK) & (rank < FIRST_COARSE_RANK + COARSE_RANKS)
    after = lax.rem(slot + 1, tm_size)
    before = lax.rem(slot + tm_size - 1, tm_size)

    def loads(tile):
        body = pl.ds(8, ROWS)
        return (
            pltpu.make_async_copy(start_hbm.at[:, :, columns(tile)], fields.at[tile, pl.ds(0, 2), body, :], load_sem.at[tile, 0]),
            pltpu.make_async_copy(nodes_hbm.at[:, :, columns(tile)], fields.at[tile, pl.ds(2, 4), body, :], load_sem.at[tile, 1]),
        )

    for tile in range(TILES):
        for copy in loads(tile):
            copy.start()

    barrier = pltpu.get_barrier_semaphore()

    @pl.when(rank > 0)
    def _():
        pl.semaphore_signal(barrier, inc=1, device_id={"tm": slot, "space": rank - 1}, device_id_type=MESH)

    @pl.when(rank < space_size - 1)
    def _():
        pl.semaphore_signal(barrier, inc=1, device_id={"tm": slot, "space": rank + 1}, device_id_type=MESH)

    @pl.when(jnp.logical_not(coarse))
    def _():
        pl.semaphore_signal(barrier, inc=1, device_id={"tm": before, "space": rank}, device_id_type=MESH)

    @pl.when(coarse)
    def _():
        def greet(step, carry):
            pl.semaphore_signal(barrier, inc=1, device_id={"tm": lax.rem(slot + step, tm_size), "space": rank}, device_id_type=MESH)
            return carry

        lax.fori_loop(1, tm_size, greet, 0)

    mixed[:, :, pl.ds(8, 8), :] = jnp.zeros((TILES, 2, 8, LANES), F32)
    mixed[:, :, pl.ds(144, 8), :] = jnp.zeros((TILES, 2, 8, LANES), F32)

    for tile in range(TILES):
        for copy in loads(tile):
            copy.wait()

    @pl.when((rank == 0) | (rank == space_size - 1))
    def _():
        pl.semaphore_wait(barrier, 2)

    @pl.when((rank > 0) & (rank < space_size - 1) & jnp.logical_not(coarse))
    def _():
        pl.semaphore_wait(barrier, 3)

    @pl.when(coarse)
    def _():
        pl.semaphore_wait(barrier, tm_size + 1)

    def halo(side):
        low, high = (ROWS, 0) if side == 0 else (8, ROWS + 8)
        return pltpu.make_async_remote_copy(
            src_ref=fields.at[:, :, pl.ds(low, 8), :], dst_ref=fields.at[:, :, pl.ds(high, 8), :],
            send_sem=halo_send.at[side], recv_sem=halo_recv.at[side],
            device_id={"tm": slot, "space": rank + 1 if side == 0 else rank - 1}, device_id_type=MESH)

    @pl.when(rank < space_size - 1)
    def _():
        halo(0).start()

    @pl.when(rank > 0)
    def _():
        halo(1).start()

    def bulk(rows, cols):
        return pltpu.make_async_remote_copy(
            src_ref=nodes_out.at[pl.ds(2, 2), rows, cols], dst_ref=next_out.at[:, rows, cols],
            send_sem=bulk_send, recv_sem=bulk_recv,
            device_id={"tm": after, "space": rank}, device_id_type=MESH)

    def field(tile, plane, low, high):
        return fields[tile, plane, pl.ds(low + 8, high - low), :]

    def mix(tile, low, high):
        for part in range(2):
            mixed[tile, part, pl.ds(low + 16, high - low), :] = (
                (5.0 / 24.0) * field(tile, part, low, high) + (1.0 / 3.0) * field(tile, 2 + part, low, high)
                - (1.0 / 24.0) * field(tile, 4 + part, low, high))

    def beside(ref, lead, low, high):
        count = high - low
        real = ref[(*lead, 0, pl.ds(low + 15, count), slice(None))] + ref[(*lead, 0, pl.ds(low + 17, count), slice(None))]
        imag = ref[(*lead, 1, pl.ds(low + 15, count), slice(None))] + ref[(*lead, 1, pl.ds(low + 17, count), slice(None))]
        return real, imag

    def rates(tile, low, high):
        return rate_of(rank * ROWS + low, tile * LANES, high - low)

    def one(tile, low, high, scale=None, keep=False):
        rate_real, rate_imag, factor = rates(tile, low, high)
        inv_real, inv_imag = inverse(1.0 - 0.5 * rate_real, -0.5 * rate_imag)
        sum_real, sum_imag = beside(mixed, (tile,), low, high)
        begin = [field(tile, part, low, high) for part in range(2)]
        old_one = [field(tile, 2 + part, low, high) for part in range(2)]
        old_two = [field(tile, 4 + part, low, high) for part in range(2)]
        own = [(5.0 / 24.0) * begin[i] - (1.0 / 6.0) * old_one[i] - (1.0 / 24.0) * old_two[i] for i in range(2)]
        top = times(rate_real, rate_imag, *own)
        node = times(inv_real, inv_imag, begin[0] + top[0] + factor * sum_imag, begin[1] + top[1] - factor * sum_real)
        if scale is not None:
            node = [part * scale for part in node]
        for i in range(2):
            staged[tile, i, pl.ds(low + 16, high - low), :] = (
                (5.0 / 24.0) * old_two[i] - (1.0 / 24.0) * begin[i] - (1.0 / 6.0) * old_one[i] + 0.5 * node[i])
            if keep:
                node_one_buf[i, pl.ds(low + 16, high - low), :] = node[i]
            first, last = max(low, 0), min(high, ROWS)
            if first < last:
                nodes_out[i, pl.ds(first, last - first), columns(tile)] = node[i][first - low:last - low]

    def two(tile, low, high, keep=False):
        rate_real, rate_imag, factor = rates(tile, low, high)
        inv_real, inv_imag = inverse(1.0 - 0.5 * rate_real, -0.5 * rate_imag)
        sum_real, sum_imag = beside(staged, (tile,), low, high)
        begin = [field(tile, part, low, high) for part in range(2)]
        old_one = [field(tile, 2 + part, low, high) for part in range(2)]
        old_two = [field(tile, 4 + part, low, high) for part in range(2)]
        if keep:
            node = [node_one_buf[i, pl.ds(low + 16, high - low), :] for i in range(2)]
        else:
            node = [nodes_out[i, pl.ds(low, high - low), columns(tile)] for i in range(2)]
        own = [(1.0 / 3.0) * old_one[i] - (1.0 / 24.0) * begin[i] - (7.0 / 24.0) * old_two[i] for i in range(2)]
        top = times(rate_real, rate_imag, *own)
        last_node = times(inv_real, inv_imag, node[0] + top[0] + factor * sum_imag, node[1] + top[1] - factor * sum_real)
        for i in range(2):
            if keep:
                whole[i, pl.ds(low + 16, high - low), :] = (
                    (1.0 / 6.0) * begin[i] + (2.0 / 3.0) * node[i] + (1.0 / 6.0) * last_node[i])
            first, last = max(low, 0), min(high, ROWS)
            if first < last:
                nodes_out[2 + i, pl.ds(first, last - first), columns(tile)] = last_node[i][first - low:last - low]

    def inner(tile):
        for low in range(0, ROWS, 32):
            mix(tile, low, low + 32)
        for low in range(0, ROWS, 32):
            one(tile, low, low + 32)
        for low in (8, 40, 72, 104):
            two(tile, low, min(low + 32, 120))

    def rim(tile):
        mix(tile, -8, 0)
        mix(tile, ROWS, ROWS + 8)
        one(tile, -8, 8, scale=jnp.concatenate([jnp.full((8, LANES), (rank > 0).astype(F32)), jnp.ones((8, LANES), F32)]))
        one(tile, 120, 136,
            scale=jnp.concatenate([jnp.ones((8, LANES), F32), jnp.full((8, LANES), (rank < space_size - 1).astype(F32))]))
        two(tile, 0, 8)
        two(tile, 120, 128)

    def wait_halo():
        @pl.when(rank > 0)
        def _():
            halo(0).wait_recv()

        @pl.when(rank < space_size - 1)
        def _():
            halo(1).wait_recv()

        @pl.when(rank == 0)
        def _():
            fields[:, :, pl.ds(0, 8), :] = jnp.zeros((TILES, 6, 8, LANES), F32)

        @pl.when(rank == space_size - 1)
        def _():
            fields[:, :, pl.ds(ROWS + 8, 8), :] = jnp.zeros((TILES, 6, 8, LANES), F32)

    middle = pl.ds(8, 112)
    upper = pl.ds(0, 8)
    lower = pl.ds(120, 8)

    @pl.when(jnp.logical_not(coarse))
    def _():
        def step(tile, carry):
            inner(tile)
            bulk(middle, columns(tile)).start()
            return carry

        lax.fori_loop(0, TILES, step, 0)
        wait_halo()

        def edge(tile, carry):
            rim(tile)
            return carry

        lax.fori_loop(0, TILES, edge, 0)
        bulk(upper, slice(None)).start()
        bulk(lower, slice(None)).start()
        bulk(slice(None), slice(None)).wait()

    @pl.when(coarse)
    def _():
        lead = (slot == 0).astype(F32)
        group, side = slot // COARSE_TILES, lax.rem(slot, COARSE_TILES)

        def piece(index):
            return lax.rem(index, COARSE_TILES), slice(None), pl.ds(pl.multiple_of((index // COARSE_TILES) * 8, 8), 8), slice(None)

        inner(0)
        bulk(middle, columns(0)).start()
        wait_halo()

        def full(tile, carry):
            for low, high in ((-8, 24), (24, 56), (56, 88), (88, 120), (120, 136)):
                mix(tile, low, high)
            for low, high in ((-8, 24), (24, 56), (56, 88), (88, 120), (120, 136)):
                one(tile, low, high, keep=True)
            for low, high in ((-8, 24), (24, 56), (56, 88), (88, 120), (120, 136)):
                two(tile, low, high, keep=True)
            for low in range(0, ROWS, 32):
                rate_real, rate_imag, factor = rates(tile, low, low + 32)
                sum_real, sum_imag = beside(whole, (), low, low + 32)
                own = [whole[i, pl.ds(low + 16, 32), :] - nodes_out[2 + i, pl.ds(low, 32), columns(tile)] for i in range(2)]
                top = times(rate_real, rate_imag, *own)
                offset[tile - FIRST_COARSE_TILE, 0, pl.ds(low, 32), :] = top[0] + factor * sum_imag + lead * field(tile, 0, low, low + 32)
                offset[tile - FIRST_COARSE_TILE, 1, pl.ds(low, 32), :] = top[1] - factor * sum_real + lead * field(tile, 1, low, low + 32)
            return carry

        lax.fori_loop(FIRST_COARSE_TILE, FIRST_COARSE_TILE + COARSE_TILES, full, 0)

        def spread(step, carry):
            peer = lax.rem(slot + step, tm_size)
            pltpu.make_async_remote_copy(
                src_ref=offset.at[piece(peer)], dst_ref=gathered.at[slot], send_sem=gather_send, recv_sem=gather_recv,
                device_id={"tm": peer, "space": rank}, device_id_type=MESH).start()
            return carry

        lax.fori_loop(1, tm_size, spread, 0)
        gathered[slot] = offset[piece(slot)]

        def fine_tile(index):
            return jnp.where(index < FIRST_COARSE_TILE, index, index + COARSE_TILES)

        def step(index, carry):
            tile = fine_tile(index)
            inner(tile)
            bulk(middle, columns(tile)).start()
            return carry

        lax.fori_loop(1, 3, step, 0)

        some = pl.ds(0, tm_size - 1)

        def peers(source, target, send, recv):
            return pltpu.make_async_remote_copy(
                src_ref=source, dst_ref=target, send_sem=send, recv_sem=recv,
                device_id={"tm": after, "space": rank}, device_id_type=MESH)

        arrival = peers(gathered.at[some], gathered.at[some], gather_send, gather_recv)
        arrival.wait_recv()
        rate_real, rate_imag, _ = rate_of(rank * ROWS + group * 8, (FIRST_COARSE_TILE + side) * LANES, 8)
        gain = inverse(1.0 - rate_real, -rate_imag)

        def scan(index, running):
            scanned[index, 0] = running[0]
            scanned[index, 1] = running[1]
            return times(*gain, running[0] + gathered[index, 0], running[1] + gathered[index, 1])

        nothing = jnp.zeros((8, LANES), F32)
        lax.fori_loop(0, tm_size, scan, (nothing, nothing))

        def give(step, carry):
            peer = lax.rem(slot + step, tm_size)
            pltpu.make_async_remote_copy(
                src_ref=scanned.at[peer], dst_ref=begins.at[piece(slot)], send_sem=scatter_send, recv_sem=scatter_recv,
                device_id={"tm": peer, "space": rank}, device_id_type=MESH).start()
            return carry

        lax.fori_loop(1, tm_size, give, 0)
        begins[piece(slot)] = scanned[slot]
        lax.fori_loop(3, len(FINE_TILES), step, 0)

        def edge(index, carry):
            rim(fine_tile(index))
            return carry

        lax.fori_loop(0, len(FINE_TILES), edge, 0)
        left = pl.ds(0, FIRST_COARSE_TILE * LANES)
        right_start = (FIRST_COARSE_TILE + COARSE_TILES) * LANES
        right = pl.ds(right_start, KY - right_start)
        for rows in (upper, lower):
            bulk(rows, left).start()
            bulk(rows, right).start()

        back = peers(scanned.at[some], scanned.at[some], scatter_send, scatter_recv)
        back.wait_recv()
        later = 1.0 - lead

        def finish(tile, carry):
            which = tile - FIRST_COARSE_TILE
            for low in range(0, ROWS, 32):
                rows = pl.ds(low, 32)
                rate_real, rate_imag, _ = rates(tile, low, low + 32)
                inv_real, inv_imag = inverse(1.0 - rate_real, -rate_imag)
                begin_new = [begins[which, i, rows, :] for i in range(2)]
                end_new = times(inv_real, inv_imag, *[begin_new[i] + offset[which, i, rows, :] for i in range(2)])
                for i in range(2):
                    old_end = nodes_out[2 + i, rows, columns(tile)]
                    nodes_out[i, rows, columns(tile)] += 0.5 * (
                        (begin_new[i] - later * field(tile, i, low, low + 32)) + (end_new[i] - old_end))
                    nodes_out[2 + i, rows, columns(tile)] = end_new[i]
                    next_out[i, rows, columns(tile)] = begin_new[i]
            return carry

        lax.fori_loop(FIRST_COARSE_TILE, FIRST_COARSE_TILE + COARSE_TILES, finish, 0)
        arrival.wait_send()
        back.wait_send()
        sent = pl.ds(0, len(FINE_TILES) * LANES)
        bulk(slice(None), sent).wait()

    @pl.when(rank < space_size - 1)
    def _():
        halo(0).wait_send()

    @pl.when(rank > 0)
    def _():
        halo(1).wait_send()

    @pl.when(slot == 0)
    def _():
        def restore(tile, carry):
            for i in range(2):
                next_out[i, :, columns(tile)] = fields[tile, i, pl.ds(8, ROWS), :]
            return carry

        lax.fori_loop(0, TILES, restore, 0)


def solution(mesh):
    tm_size, space_size = mesh.shape["tm"], mesh.shape["space"]

    def body(start_values, node_values):
        any_space = pl.BlockSpec(memory_space=pltpu.MemorySpace.HBM)
        vmem = pl.BlockSpec(memory_space=pltpu.MemorySpace.VMEM)
        dma = pltpu.SemaphoreType.DMA
        next_start, nodes = pl.pallas_call(
            functools.partial(kernel, tm_size, space_size),
            out_shape=(pltpu.MemorySpace.VMEM((2, ROWS, KY), F32), pltpu.MemorySpace.VMEM((4, ROWS, KY), F32)),
            in_specs=[any_space, any_space],
            out_specs=(vmem, vmem),
            scratch_shapes=[
                pltpu.VMEM((TILES, 6, ROWS + 16, LANES), F32),
                pltpu.VMEM((TILES, 2, ROWS + 32, LANES), F32),
                pltpu.VMEM((TILES, 2, ROWS + 32, LANES), F32),
                pltpu.VMEM((2, ROWS + 32, LANES), F32),
                pltpu.VMEM((2, ROWS + 32, LANES), F32),
                pltpu.VMEM((COARSE_TILES, 2, ROWS, LANES), F32),
                pltpu.VMEM((tm_size, 2, 8, LANES), F32),
                pltpu.VMEM((tm_size, 2, 8, LANES), F32),
                pltpu.VMEM((COARSE_TILES, 2, ROWS, LANES), F32),
                dma((TILES, 2)),
                dma((2,)),
                dma((2,)),
                dma,
                dma,
                dma,
                dma,
                dma,
                dma,
            ],
            compiler_params=pltpu.CompilerParams(collective_id=0, has_side_effects=True, vmem_limit_bytes=61696 * 1024),
            name="pfasst",
        )(start_values[0], node_values[0].reshape(4, ROWS, KY))
        return next_start[None], nodes.reshape(1, 2, 2, ROWS, KY)

    return jax.shard_map(
        body,
        mesh=mesh,
        in_specs=(P("tm", None, "space", None), P("tm", None, None, "space", None)),
        out_specs=(P("tm", None, "space", None), P("tm", None, None, "space", None)),
        check_vma=False,
    )
```

```python
import functools

import jax
import jax.numpy as jnp
from jax import lax
from jax.experimental import pallas as pl
from jax.experimental.pallas import tpu as pltpu
from jax.sharding import PartitionSpec as P

MESH = pl.DeviceIdType.MESH
F32 = jnp.float32
KX = 1024
KY = 1024
CX = 256
LANES = 128
ROWS = 128
TILES = KY // LANES
FIRST_COARSE_TILE = (KY // 2 - CX // 2) // LANES
COARSE_TILES = CX // LANES
FIRST_COARSE_RANK = (KX // 2 - CX // 2) // ROWS
COARSE_RANKS = CX // ROWS
FINE_TILES = TILES - COARSE_TILES
RING = 4
GROUP = 16
PIECE_ROWS = COARSE_TILES * ROWS // GROUP
RELAY_SHARED = 1
RELAY_WRAP = 0
RELAYS = 2 * (2 + RELAY_SHARED + RELAY_WRAP)
RELAY_ROWS = 56
EARLY = 5
EARLY_WRAP = 5

diffusion = 1.5
drift = 0.8
shear = 0.6


def columns(tile):
    return pl.ds(pl.multiple_of(tile * LANES, LANES), LANES)


def rate_of(first_row, first_column, rows):
    row = (first_row + lax.broadcasted_iota(jnp.int32, (rows, LANES), 0)).astype(F32)
    column = (first_column + lax.broadcasted_iota(jnp.int32, (rows, LANES), 1)).astype(F32)
    along = (row - KX // 2) / (KX // 2)
    across = (column - KY // 2) / (KY // 2)
    return -diffusion * (along * along + across * across), -drift * across, shear * across


def times(ar, ai, br, bi):
    return ar * br - ai * bi, ar * bi + ai * br


def inverse(real_part, imag_part):
    scale = 1.0 / (real_part * real_part + imag_part * imag_part)
    return real_part * scale, -imag_part * scale


def tile_at(index):
    early = jnp.where(index < COARSE_TILES, index + FIRST_COARSE_TILE, index - COARSE_TILES)
    return jnp.where(index < FIRST_COARSE_TILE + COARSE_TILES, early, index)


def kernel(tm_size, space_size, start_hbm, nodes_hbm, next_out, nodes_out, fields, mixed, staged, node_one_buf, whole, offset,
           gathered, carry_in, carry_out, results, begins, first_leg, second_leg, load_sem, halo_send, halo_recv, bulk_send,
           bulk_recv, gather_send, gather_recv, carry_send, carry_recv, scatter_send, scatter_recv, relay_send, relay_recv,
           ready, ready_carry, aside, aside_send, aside_recv):
    slot = lax.axis_index("tm")
    rank = lax.axis_index("space")
    coarse = (rank >= FIRST_COARSE_RANK) & (rank < FIRST_COARSE_RANK + COARSE_RANKS)
    fine = jnp.logical_not(coarse)
    shared = (rank == FIRST_COARSE_RANK - 1) | (rank == FIRST_COARSE_RANK + COARSE_RANKS)
    column, place = slot // RING, lax.rem(slot, RING)

    def at_slot(index):
        return {"tm": lax.rem(index, tm_size), "space": rank}

    after = slot + 1
    before = slot + tm_size - 1
    above = column * RING + lax.rem(place + 1, RING)
    below = column * RING + lax.rem(place + RING - 1, RING)

    def loads(tile):
        body = pl.ds(8, ROWS)
        return (
            pltpu.make_async_copy(start_hbm.at[:, :, columns(tile)], fields.at[tile, pl.ds(0, 2), body, :], load_sem.at[tile, 0]),
            pltpu.make_async_copy(nodes_hbm.at[:, :, columns(tile)], fields.at[tile, pl.ds(2, 4), body, :], load_sem.at[tile, 1]),
        )

    def wait_load(tile):
        for copy in loads(tile):
            copy.wait()

    barrier = pltpu.get_barrier_semaphore()

    def greet(target):
        pl.semaphore_signal(barrier, inc=1, device_id=target, device_id_type=MESH)

    @pl.when(rank > 0)
    def _():
        greet({"tm": slot, "space": rank - 1})

    @pl.when(rank < space_size - 1)
    def _():
        greet({"tm": slot, "space": rank + 1})

    greet(at_slot(before))

    @pl.when(fine)
    def _():
        greet(at_slot(above))

        @pl.when(place == 0)
        def _():
            greet(at_slot(slot + tm_size - RING + 1))

    member, group = lax.rem(slot, GROUP), slot // GROUP
    groups = tm_size // GROUP
    depth = GROUP // RING

    def in_group(index):
        return at_slot(group * GROUP + index)

    def facing(step):
        return at_slot((group + step) * GROUP + (depth - 1 - member // RING) * RING + place)

    @pl.when(coarse)
    def _():
        def call(index, carry):
            greet(in_group(index))
            return carry

        lax.fori_loop(member + 1, GROUP, call, 0)

        @pl.when(group < groups - 1)
        def _():
            greet(facing(1))

    def begin_load(index, carry):
        for copy in loads(tile_at(index)):
            copy.start()
        return carry

    lax.fori_loop(0, TILES, begin_load, 0)
    mixed[:, :, pl.ds(8, 8), :] = jnp.zeros((TILES, 2, 8, LANES), F32)
    mixed[:, :, pl.ds(144, 8), :] = jnp.zeros((TILES, 2, 8, LANES), F32)

    with jax.named_scope("load"):
        for tile in range(FIRST_COARSE_TILE, FIRST_COARSE_TILE + COARSE_TILES):
            wait_load(tile)

    def count(flag):
        return flag.astype(jnp.int32)

    with jax.named_scope("barrier"):
        own_kind = jnp.where(coarse, member + count(group > 0), 1 + count(place == 1))
        pl.semaphore_wait(barrier, 1 + count(rank > 0) + count(rank < space_size - 1) + own_kind)

    @pl.when(coarse)
    def _():
        @pl.when(group > 0)
        def _():
            pl.semaphore_signal(ready_carry, inc=1, device_id=facing(-1), device_id_type=MESH)

        def answer(index, carry):
            pl.semaphore_signal(ready, inc=1, device_id=in_group(index), device_id_type=MESH)
            return carry

        lax.fori_loop(0, member, answer, 0)

    parts = (pl.ds(FIRST_COARSE_TILE, COARSE_TILES), pl.ds(0, FIRST_COARSE_TILE),
             pl.ds(FIRST_COARSE_TILE + COARSE_TILES, TILES - FIRST_COARSE_TILE - COARSE_TILES))

    def halo(side, part):
        low, high = (ROWS, 0) if side == 0 else (8, ROWS + 8)
        return pltpu.make_async_remote_copy(
            src_ref=fields.at[parts[part], :, pl.ds(low, 8), :], dst_ref=fields.at[parts[part], :, pl.ds(high, 8), :],
            send_sem=halo_send.at[side, part], recv_sem=halo_recv.at[side, part],
            device_id={"tm": slot, "space": rank + 1 if side == 0 else rank - 1}, device_id_type=MESH)

    def send_halo(*which):
        @pl.when(rank < space_size - 1)
        def _():
            for part in which:
                halo(0, part).start()

        @pl.when(rank > 0)
        def _():
            for part in which:
                halo(1, part).start()

    def wait_halo(*which):
        @pl.when(rank > 0)
        def _():
            for part in which:
                halo(0, part).wait_recv()

        @pl.when(rank < space_size - 1)
        def _():
            for part in which:
                halo(1, part).wait_recv()

    send_halo(0)

    def bulk(rows, cols, index=0):
        return pltpu.make_async_remote_copy(
            src_ref=nodes_out.at[pl.ds(2, 2), rows, cols], dst_ref=next_out.at[:, rows, cols],
            send_sem=bulk_send.at[index], recv_sem=bulk_recv, device_id=at_slot(after), device_id_type=MESH)

    def push(rows, cols, index):
        @pl.when(slot < tm_size - 1)
        def _():
            bulk(rows, cols, index).start()

    def field(tile, plane, low, high):
        return fields[tile, plane, pl.ds(low + 8, high - low), :]

    def mix(tile, low, high):
        for part in range(2):
            mixed[tile, part, pl.ds(low + 16, high - low), :] = (
                (5.0 / 24.0) * field(tile, part, low, high) + (1.0 / 3.0) * field(tile, 2 + part, low, high)
                - (1.0 / 24.0) * field(tile, 4 + part, low, high))

    def beside(ref, lead, low, high):
        count = high - low
        real = ref[(*lead, 0, pl.ds(low + 15, count), slice(None))] + ref[(*lead, 0, pl.ds(low + 17, count), slice(None))]
        imag = ref[(*lead, 1, pl.ds(low + 15, count), slice(None))] + ref[(*lead, 1, pl.ds(low + 17, count), slice(None))]
        return real, imag

    def rates(tile, low, high):
        return rate_of(rank * ROWS + low, tile * LANES, high - low)

    def one(tile, low, high, scale=None, keep=False):
        rate_real, rate_imag, factor = rates(tile, low, high)
        inv_real, inv_imag = inverse(1.0 - 0.5 * rate_real, -0.5 * rate_imag)
        sum_real, sum_imag = beside(mixed, (tile,), low, high)
        begin = [field(tile, part, low, high) for part in range(2)]
        old_one = [field(tile, 2 + part, low, high) for part in range(2)]
        old_two = [field(tile, 4 + part, low, high) for part in range(2)]
        own = [(5.0 / 24.0) * begin[i] - (1.0 / 6.0) * old_one[i] - (1.0 / 24.0) * old_two[i] for i in range(2)]
        top = times(rate_real, rate_imag, *own)
        node = times(inv_real, inv_imag, begin[0] + top[0] + factor * sum_imag, begin[1] + top[1] - factor * sum_real)
        if scale is not None:
            node = [part * scale for part in node]
        for i in range(2):
            staged[tile, i, pl.ds(low + 16, high - low), :] = (
                (5.0 / 24.0) * old_two[i] - (1.0 / 24.0) * begin[i] - (1.0 / 6.0) * old_one[i] + 0.5 * node[i])
            if keep:
                node_one_buf[i, pl.ds(low + 16, high - low), :] = node[i]
            first, last = max(low, 0), min(high, ROWS)
            if first < last:
                nodes_out[i, pl.ds(first, last - first), columns(tile)] = node[i][first - low:last - low]

    def two(tile, low, high, keep=False):
        rate_real, rate_imag, factor = rates(tile, low, high)
        inv_real, inv_imag = inverse(1.0 - 0.5 * rate_real, -0.5 * rate_imag)
        sum_real, sum_imag = beside(staged, (tile,), low, high)
        begin = [field(tile, part, low, high) for part in range(2)]
        old_one = [field(tile, 2 + part, low, high) for part in range(2)]
        old_two = [field(tile, 4 + part, low, high) for part in range(2)]
        if keep:
            node = [node_one_buf[i, pl.ds(low + 16, high - low), :] for i in range(2)]
        else:
            node = [nodes_out[i, pl.ds(low, high - low), columns(tile)] for i in range(2)]
        own = [(1.0 / 3.0) * old_one[i] - (1.0 / 24.0) * begin[i] - (7.0 / 24.0) * old_two[i] for i in range(2)]
        top = times(rate_real, rate_imag, *own)
        last_node = times(inv_real, inv_imag, node[0] + top[0] + factor * sum_imag, node[1] + top[1] - factor * sum_real)
        for i in range(2):
            if keep:
                whole[i, pl.ds(low + 16, high - low), :] = (
                    (1.0 / 6.0) * begin[i] + (2.0 / 3.0) * node[i] + (1.0 / 6.0) * last_node[i])
            first, last = max(low, 0), min(high, ROWS)
            if first < last:
                nodes_out[2 + i, pl.ds(first, last - first), columns(tile)] = last_node[i][first - low:last - low]

    def inner(tile):
        for low in range(0, ROWS, 32):
            mix(tile, low, low + 32)
        for low in range(0, ROWS, 32):
            one(tile, low, low + 32)
        for low in (8, 40, 72, 104):
            two(tile, low, min(low + 32, 120))

    def rim(tile):
        mix(tile, -8, 0)
        mix(tile, ROWS, ROWS + 8)
        one(tile, -8, 8, scale=jnp.concatenate([jnp.full((8, LANES), (rank > 0).astype(F32)), jnp.ones((8, LANES), F32)]))
        one(tile, 120, 136,
            scale=jnp.concatenate([jnp.ones((8, LANES), F32), jnp.full((8, LANES), (rank < space_size - 1).astype(F32))]))
        two(tile, 0, 8)
        two(tile, 120, 128)

    middle = pl.ds(8, 112)
    upper = pl.ds(0, 8)
    lower = pl.ds(120, 8)

    def inner_push(index, carry):
        tile = tile_at(index)
        wait_load(tile)
        inner(tile)
        push(middle, columns(tile), index)
        return carry

    def edge(index, carry):
        rim(tile_at(index))
        return carry

    def settle(cols):
        @pl.when(slot > 0)
        def _():
            bulk(slice(None), cols).wait_recv()

    @pl.when(fine)
    def _():
        def relay_source(chunk):
            rows = pl.ds(pl.multiple_of(8 + lax.rem(chunk, 2) * RELAY_ROWS, 8), RELAY_ROWS)
            return rows, columns(tile_at(chunk // 2))

        def leg(which, chunk):
            rows, cols = relay_source(chunk)
            if which == 0:
                source, target, device = nodes_out.at[pl.ds(2, 2), rows, cols], first_leg.at[chunk], at_slot(below)
                recv = relay_recv.at[0, chunk]
            elif which == 1:
                source, target, device, recv = first_leg.at[chunk], second_leg.at[chunk], at_slot(below), relay_recv.at[1, chunk]
            else:
                origin = column * RING + lax.rem(place + 2, RING)
                source, target, device, recv = second_leg.at[chunk], next_out.at[:, rows, cols], at_slot(origin + 1), bulk_recv
            return pltpu.make_async_remote_copy(
                src_ref=source, dst_ref=target, send_sem=relay_send.at[which, chunk], recv_sem=recv,
                device_id=device, device_id_type=MESH)

        def relayed(which):
            start = lax.rem(place + which, RING)
            wraps = (start == RING - 1).astype(jnp.int32)
            return 2 + RELAY_SHARED * shared.astype(jnp.int32) + RELAY_WRAP * wraps

        def has_origin(which):
            return column * RING + lax.rem(place + which, RING) < tm_size - 1

        def start_tile(index, carry):
            @pl.when(index >= COARSE_TILES)
            def _():
                wait_load(tile_at(index))

            inner(tile_at(index))

            @pl.when(has_origin(0) & (index < relayed(0)))
            def _():
                leg(0, 2 * index).start()
                leg(0, 2 * index + 1).start()

            @pl.when(has_origin(0) & (index >= relayed(0)))
            def _():
                bulk(middle, columns(tile_at(index)), index).start()

            return carry

        def forward(which, chunk):
            @pl.when(has_origin(which) & (chunk < 2 * relayed(which)))
            def _():
                leg(which - 1, chunk).wait_recv()
                leg(which, chunk).start()

        with jax.named_scope("inner"):
            lax.fori_loop(0, TILES, start_tile, 0)
        send_halo(1, 2)
        with jax.named_scope("fwdA"):
            forward(1, 0)
            forward(1, 1)
        with jax.named_scope("halo"):
            wait_halo(0, 1, 2)

        @pl.when(rank == 0)
        def _():
            fields[:, :, pl.ds(0, 8), :] = jnp.zeros((TILES, 6, 8, LANES), F32)

        @pl.when(rank == space_size - 1)
        def _():
            fields[:, :, pl.ds(ROWS + 8, 8), :] = jnp.zeros((TILES, 6, 8, LANES), F32)

        with jax.named_scope("rim"):
            lax.fori_loop(0, TILES, edge, 0)
        push(upper, slice(None), TILES)
        push(lower, slice(None), TILES + 1)

        def pass_on(step, carry):
            forward(1, step)
            forward(2, step - 2)
            return carry

        with jax.named_scope("fwdB"):
            lax.fori_loop(2, RELAYS + 2, pass_on, 0)
        with jax.named_scope("settle"):
            settle(slice(None))

        @pl.when(slot < tm_size - 1)
        def _():
            def sent(index, carry):
                @pl.when(index >= relayed(0))
                def _():
                    bulk(middle, columns(tile_at(index)), index).wait_send()

                return carry

            lax.fori_loop(0, TILES, sent, 0)
            bulk(upper, slice(None), TILES).wait_send()
            bulk(lower, slice(None), TILES + 1).wait_send()

        for which in range(3):
            def legs_sent(chunk, carry):
                @pl.when(has_origin(which) & (chunk < 2 * relayed(which)))
                def _():
                    leg(which, chunk).wait_send()

                return carry

            lax.fori_loop(0, RELAYS, legs_sent, 0)

    @pl.when(coarse)
    def _():
        lead = (slot == 0).astype(F32)

        def piece(index):
            row = index // RING
            number = jnp.where(lax.rem(group, 2) == 1, depth - 1 - row, row) * RING + lax.rem(index, RING)
            share = GROUP // COARSE_TILES
            rows = pl.ds(pl.multiple_of(lax.rem(number, share) * PIECE_ROWS, 8), PIECE_ROWS)
            return number // share, slice(None), rows, slice(None)

        def inner_only(index, carry):
            inner(tile_at(index))
            return carry

        def push_only(index, carry):
            push(middle, columns(tile_at(index)), index)
            return carry

        lax.fori_loop(COARSE_TILES, TILES, lambda index, carry: (wait_load(tile_at(index)), carry)[1], 0)
        send_halo(1, 2)
        with jax.named_scope("innerA"):
            lax.fori_loop(COARSE_TILES, TILES, inner_only, 0)
        with jax.named_scope("halo"):
            wait_halo(0)

        def full(tile, carry):
            bands = ((-8, 24), (24, 56), (56, 88), (88, 120), (120, 136))
            for low, high in bands:
                mix(tile, low, high)
            for low, high in bands:
                one(tile, low, high, keep=True)
            for low, high in bands:
                two(tile, low, high, keep=True)
            for low in range(0, ROWS, 32):
                rate_real, rate_imag, factor = rates(tile, low, low + 32)
                sum_real, sum_imag = beside(whole, (), low, low + 32)
                own = [whole[i, pl.ds(low + 16, 32), :] - nodes_out[2 + i, pl.ds(low, 32), columns(tile)] for i in range(2)]
                top = times(rate_real, rate_imag, *own)
                offset[tile - FIRST_COARSE_TILE, 0, pl.ds(low, 32), :] = top[0] + factor * sum_imag + lead * field(tile, 0, low, low + 32)
                offset[tile - FIRST_COARSE_TILE, 1, pl.ds(low, 32), :] = top[1] - factor * sum_real + lead * field(tile, 1, low, low + 32)
            return carry

        def gather(source, target):
            return pltpu.make_async_remote_copy(
                src_ref=offset.at[piece(target)], dst_ref=gathered.at[source], send_sem=gather_send.at[target],
                recv_sem=gather_recv.at[source], device_id=in_group(target), device_id_type=MESH)

        def scatter(source, target):
            return pltpu.make_async_remote_copy(
                src_ref=results.at[target], dst_ref=begins.at[piece(source)], send_sem=scatter_send.at[target],
                recv_sem=scatter_recv.at[source], device_id=in_group(target), device_id_type=MESH)

        def hand_on():
            return pltpu.make_async_remote_copy(
                src_ref=carry_out, dst_ref=carry_in, send_sem=carry_send, recv_sem=carry_recv, device_id=facing(1),
                device_id_type=MESH)

        row = member // RING
        beside_row = (row + 1 - 2 * lax.rem(row, 2)) * RING

        def detour(stage):
            source = offset.at[piece(row * RING)] if stage == 0 else results.at[row * RING]
            sem = gather_send if stage == 0 else scatter_send
            return pltpu.make_async_remote_copy(
                src_ref=source, dst_ref=aside.at[stage], send_sem=sem.at[row * RING], recv_sem=aside_recv.at[stage],
                device_id=in_group(beside_row), device_id_type=MESH)

        def relay_aside(stage):
            origin = beside_row + RING - 1
            target = gathered.at[origin] if stage == 0 else begins.at[piece(origin)]
            sem = gather_recv if stage == 0 else scatter_recv
            return pltpu.make_async_remote_copy(
                src_ref=aside.at[stage], dst_ref=target, send_sem=aside_send.at[stage], recv_sem=sem.at[origin],
                device_id=in_group(beside_row), device_id_type=MESH)

        def pass_aside(stage):
            @pl.when(place == 0)
            def _():
                detour(stage).wait_recv()
                relay_aside(stage).start()

        def blocked(target):
            return (place == RING - 1) & (target == row * RING)

        def other(distance):
            return lax.rem(member + distance, GROUP)

        with jax.named_scope("full"):
            lax.fori_loop(FIRST_COARSE_TILE, FIRST_COARSE_TILE + COARSE_TILES, full, 0)
        with jax.named_scope("ready"):
            @pl.when(member < GROUP - 1)
            def _():
                pl.semaphore_wait(ready, GROUP - 1 - member)

        def spread(distance, carry):
            @pl.when(jnp.logical_not(blocked(other(distance))))
            def _():
                gather(member, other(distance)).start()

            return carry

        with jax.named_scope("spread"):
            @pl.when(place == RING - 1)
            def _():
                detour(0).start()

            lax.fori_loop(1, GROUP, spread, 0)
        gathered[member] = offset[piece(member)]
        early = jnp.where(place == RING - 1, EARLY_WRAP, EARLY)
        lax.fori_loop(COARSE_TILES, early, push_only, 0)
        tile, _, _, _ = piece(member)
        number = jnp.where(lax.rem(group, 2) == 1, depth - 1 - member // RING, member // RING) * RING + place
        first = lax.rem(number, GROUP // COARSE_TILES) * PIECE_ROWS
        rate_real, rate_imag, _ = rate_of(rank * ROWS + first, (FIRST_COARSE_TILE + tile) * LANES, PIECE_ROWS)
        gain = inverse(1.0 - rate_real, -rate_imag)

        with jax.named_scope("aside0"):
            pass_aside(0)
        with jax.named_scope("gather"):
            def arrive(distance, carry):
                gather(other(distance), member).wait_recv()
                return carry

            lax.fori_loop(1, GROUP, arrive, 0)

        with jax.named_scope("carry"):
            @pl.when(group == 0)
            def _():
                carry_in[...] = jnp.zeros((2, PIECE_ROWS, LANES), F32)

            @pl.when(group > 0)
            def _():
                hand_on().wait_recv()

        def scan(index, running):
            for i in range(2):
                results[index, i] = running[i]
            return times(*gain, running[0] + gathered[index, 0], running[1] + gathered[index, 1])

        with jax.named_scope("scan"):
            running = lax.fori_loop(0, GROUP, scan, (carry_in[0], carry_in[1]))
            for i in range(2):
                carry_out[i] = running[i]

            @pl.when(group < groups - 1)
            def _():
                pl.semaphore_wait(ready_carry, 1)
                hand_on().start()

        def give(distance, carry):
            @pl.when(jnp.logical_not(blocked(other(distance))))
            def _():
                scatter(member, other(distance)).start()

            return carry

        with jax.named_scope("give"):
            @pl.when(place == RING - 1)
            def _():
                detour(1).start()

            lax.fori_loop(1, GROUP, give, 0)
        begins[piece(member)] = results[member]
        lax.fori_loop(early, TILES, push_only, 0)
        with jax.named_scope("halo2"):
            wait_halo(1, 2)
        with jax.named_scope("rim"):
            lax.fori_loop(COARSE_TILES, TILES, edge, 0)
        left = pl.ds(0, FIRST_COARSE_TILE * LANES)
        right_start = (FIRST_COARSE_TILE + COARSE_TILES) * LANES
        right = pl.ds(right_start, KY - right_start)
        rims = [(upper, left), (upper, right), (lower, left), (lower, right)]
        for number, (rows, cols) in enumerate(rims):
            push(rows, cols, TILES + number)

        with jax.named_scope("aside1"):
            pass_aside(1)
        with jax.named_scope("back"):
            def fetch(distance, carry):
                scatter(other(distance), member).wait_recv()
                return carry

            lax.fori_loop(1, GROUP, fetch, 0)

        later = 1.0 - lead

        def finish(tile, carry):
            which = tile - FIRST_COARSE_TILE
            for low in range(0, ROWS, 32):
                rows = pl.ds(low, 32)
                rate_real, rate_imag, _ = rates(tile, low, low + 32)
                inv_real, inv_imag = inverse(1.0 - rate_real, -rate_imag)
                begin_new = [begins[which, i, rows, :] for i in range(2)]
                end_new = times(inv_real, inv_imag, *[begin_new[i] + offset[which, i, rows, :] for i in range(2)])
                for i in range(2):
                    old_end = nodes_out[2 + i, rows, columns(tile)]
                    nodes_out[i, rows, columns(tile)] += 0.5 * (
                        (begin_new[i] - later * field(tile, i, low, low + 32)) + (end_new[i] - old_end))
                    nodes_out[2 + i, rows, columns(tile)] = end_new[i]
                    next_out[i, rows, columns(tile)] = begin_new[i]
            return carry

        with jax.named_scope("finish"):
            lax.fori_loop(FIRST_COARSE_TILE, FIRST_COARSE_TILE + COARSE_TILES, finish, 0)

        with jax.named_scope("settle"):
            settle(pl.ds(0, FINE_TILES * LANES))

        @pl.when(slot < tm_size - 1)
        def _():
            def sent(index, carry):
                bulk(middle, columns(tile_at(index)), index).wait_send()
                return carry

            lax.fori_loop(COARSE_TILES, TILES, sent, 0)
            for number, (rows, cols) in enumerate(rims):
                bulk(rows, cols, TILES + number).wait_send()

        @pl.when(group < groups - 1)
        def _():
            hand_on().wait_send()

        def let_go(distance, carry):
            gather(member, other(distance)).wait_send()
            scatter(member, other(distance)).wait_send()
            return carry

        lax.fori_loop(1, GROUP, let_go, 0)

        @pl.when(place == 0)
        def _():
            for stage in range(2):
                relay_aside(stage).wait_send()

    @pl.when(rank < space_size - 1)
    def _():
        for part in range(3):
            halo(0, part).wait_send()

    @pl.when(rank > 0)
    def _():
        for part in range(3):
            halo(1, part).wait_send()

    @pl.when(slot == 0)
    def _():
        def restore(tile, carry):
            for i in range(2):
                next_out[i, :, columns(tile)] = fields[tile, i, pl.ds(8, ROWS), :]
            return carry

        lax.fori_loop(0, TILES, restore, 0)


def deliver(start_ref, nodes_ref, start_hbm, nodes_hbm, sems):
    copies = [pltpu.make_async_copy(nodes_ref.at[i], nodes_hbm.at[i], sems.at[i]) for i in range(4)]
    copies += [pltpu.make_async_copy(start_ref.at[i], start_hbm.at[i], sems.at[4 + i]) for i in range(2)]
    for copy in copies:
        copy.start()
    for copy in copies:
        copy.wait()


def solution(mesh):
    tm_size, space_size = mesh.shape["tm"], mesh.shape["space"]

    def body(start_values, node_values):
        hbm = pl.BlockSpec(memory_space=pltpu.MemorySpace.HBM)
        vmem = pl.BlockSpec(memory_space=pltpu.MemorySpace.VMEM)
        dma = pltpu.SemaphoreType.DMA
        next_start, nodes = pl.pallas_call(
            functools.partial(kernel, tm_size, space_size),
            out_shape=(pltpu.MemorySpace.VMEM((2, ROWS, KY), F32), pltpu.MemorySpace.VMEM((4, ROWS, KY), F32)),
            in_specs=[hbm, hbm],
            out_specs=(vmem, vmem),
            scratch_shapes=[
                pltpu.VMEM((TILES, 6, ROWS + 16, LANES), F32),
                pltpu.VMEM((TILES, 2, ROWS + 32, LANES), F32),
                pltpu.VMEM((TILES, 2, ROWS + 32, LANES), F32),
                pltpu.VMEM((2, ROWS + 32, LANES), F32),
                pltpu.VMEM((2, ROWS + 32, LANES), F32),
                pltpu.VMEM((COARSE_TILES, 2, ROWS, LANES), F32),
                pltpu.VMEM((GROUP, 2, PIECE_ROWS, LANES), F32),
                pltpu.VMEM((2, PIECE_ROWS, LANES), F32),
                pltpu.VMEM((2, PIECE_ROWS, LANES), F32),
                pltpu.VMEM((GROUP, 2, PIECE_ROWS, LANES), F32),
                pltpu.VMEM((COARSE_TILES, 2, ROWS, LANES), F32),
                pltpu.VMEM((RELAYS, 2, RELAY_ROWS, LANES), F32),
                pltpu.VMEM((RELAYS, 2, RELAY_ROWS, LANES), F32),
                dma((TILES, 2)),
                dma((2, 3)),
                dma((2, 3)),
                dma((TILES + 4,)),
                dma,
                dma((GROUP,)),
                dma((GROUP,)),
                dma,
                dma,
                dma((GROUP,)),
                dma((GROUP,)),
                dma((3, RELAYS)),
                dma((2, RELAYS)),
                pltpu.SemaphoreType.REGULAR,
                pltpu.SemaphoreType.REGULAR,
                pltpu.VMEM((2, 2, PIECE_ROWS, LANES), F32),
                dma((2,)),
                dma((2,)),
            ],
            compiler_params=pltpu.CompilerParams(collective_id=0, has_side_effects=True, vmem_limit_bytes=61696 * 1024),
            name="pfasst",
        )(start_values[0], node_values[0].reshape(4, ROWS, KY))
        next_start, nodes = pl.pallas_call(
            deliver,
            out_shape=(jax.ShapeDtypeStruct((2, ROWS, KY), F32), jax.ShapeDtypeStruct((4, ROWS, KY), F32)),
            in_specs=[vmem, vmem],
            out_specs=(hbm, hbm),
            scratch_shapes=[dma((6,))],
            compiler_params=pltpu.CompilerParams(vmem_limit_bytes=2**20),
            name="deliver",
        )(next_start, nodes)
        return next_start[None], nodes.reshape(1, 2, 2, ROWS, KY)

    return jax.shard_map(
        body,
        mesh=mesh,
        in_specs=(P("tm", None, "space", None), P("tm", None, None, "space", None)),
        out_specs=(P("tm", None, "space", None), P("tm", None, None, "space", None)),
        check_vma=False,
    )
```

```python
import functools

import jax
import jax.numpy as jnp
from jax import lax
from jax.experimental import pallas as pl
from jax.experimental.pallas import tpu as pltpu
from jax.sharding import PartitionSpec as P

MESH = pl.DeviceIdType.MESH
F32 = jnp.float32
KX = 1024
KY = 1024
CX = 256
LANES = 128
ROWS = 128
TILES = KY // LANES
FIRST_COARSE_TILE = (KY // 2 - CX // 2) // LANES
COARSE_TILES = CX // LANES
FIRST_COARSE_RANK = (KX // 2 - CX // 2) // ROWS
COARSE_RANKS = CX // ROWS
FINE_TILES = TILES - COARSE_TILES
RING = 4
GROUP = 8
PIECE_ROWS = COARSE_TILES * ROWS // GROUP
RELAY_SHARED = 1
RELAY_WRAP = 0
RELAY_BOTH = 1
RELAYS = 2 * (2 + RELAY_SHARED + RELAY_WRAP + RELAY_BOTH)
RELAY_ROWS = 56
EARLY = 4
EARLY_WRAP = 3
EARLY_STEP = 4
WRAP_STEP = 3
LEAD = 1
ASIDE_GROUPS = 2
FIRST = 2
FIRST_WRAP = 1

diffusion = 1.5
drift = 0.8
shear = 0.6


def columns(tile):
    return pl.ds(pl.multiple_of(tile * LANES, LANES), LANES)


def rate_of(first_row, first_column, rows):
    row = (first_row + lax.broadcasted_iota(jnp.int32, (rows, LANES), 0)).astype(F32)
    column = (first_column + lax.broadcasted_iota(jnp.int32, (rows, LANES), 1)).astype(F32)
    along = (row - KX // 2) / (KX // 2)
    across = (column - KY // 2) / (KY // 2)
    return -diffusion * (along * along + across * across), -drift * across, shear * across


def times(ar, ai, br, bi):
    return ar * br - ai * bi, ar * bi + ai * br


def inverse(real_part, imag_part):
    scale = 1.0 / (real_part * real_part + imag_part * imag_part)
    return real_part * scale, -imag_part * scale


def tile_at(index):
    early = jnp.where(index < COARSE_TILES, index + FIRST_COARSE_TILE, index - COARSE_TILES)
    return jnp.where(index < FIRST_COARSE_TILE + COARSE_TILES, early, index)


def kernel(tm_size, space_size, start_hbm, nodes_hbm, next_out, nodes_out, fields, mixed, staged, node_one_buf, whole, offset,
           gathered, carry_in, carry_out, results, begins, first_leg, second_leg, load_sem, halo_send, halo_recv, bulk_send,
           bulk_recv, gather_send, gather_recv, carry_send, carry_recv, scatter_send, scatter_recv, relay_send, relay_recv,
           ready, ready_carry, aside, aside_send, aside_recv):
    slot = lax.axis_index("tm")
    rank = lax.axis_index("space")
    coarse = (rank >= FIRST_COARSE_RANK) & (rank < FIRST_COARSE_RANK + COARSE_RANKS)
    fine = jnp.logical_not(coarse)
    shared = (rank == FIRST_COARSE_RANK - 1) | (rank == FIRST_COARSE_RANK + COARSE_RANKS)
    column, place = slot // RING, lax.rem(slot, RING)

    def at_slot(index):
        return {"tm": lax.rem(index, tm_size), "space": rank}

    after = slot + 1
    before = slot + tm_size - 1
    above = column * RING + lax.rem(place + 1, RING)
    below = column * RING + lax.rem(place + RING - 1, RING)

    def loads(tile):
        body = pl.ds(8, ROWS)
        return (
            pltpu.make_async_copy(start_hbm.at[:, :, columns(tile)], fields.at[tile, pl.ds(0, 2), body, :], load_sem.at[tile, 0]),
            pltpu.make_async_copy(nodes_hbm.at[:, :, columns(tile)], fields.at[tile, pl.ds(2, 4), body, :], load_sem.at[tile, 1]),
        )

    def wait_load(tile):
        for copy in loads(tile):
            copy.wait()

    barrier = pltpu.get_barrier_semaphore()

    def greet(target):
        pl.semaphore_signal(barrier, inc=1, device_id=target, device_id_type=MESH)

    @pl.when(rank > 0)
    def _():
        greet({"tm": slot, "space": rank - 1})

    @pl.when(rank < space_size - 1)
    def _():
        greet({"tm": slot, "space": rank + 1})

    greet(at_slot(before))

    @pl.when(fine)
    def _():
        greet(at_slot(above))

        @pl.when(place == 0)
        def _():
            greet(at_slot(slot + tm_size - RING + 1))

    member, group = lax.rem(slot, GROUP), slot // GROUP
    groups = tm_size // GROUP
    depth = GROUP // RING

    def in_group(index):
        return at_slot(group * GROUP + index)

    def facing(step):
        return at_slot((group + step) * GROUP + (depth - 1 - member // RING) * RING + place)

    @pl.when(coarse)
    def _():
        def call(index, carry):
            greet(in_group(index))
            return carry

        lax.fori_loop(member + 1, GROUP, call, 0)

        @pl.when(group < groups - 1)
        def _():
            greet(facing(1))

    def begin_load(index, carry):
        for copy in loads(tile_at(index)):
            copy.start()
        return carry

    lax.fori_loop(0, TILES, begin_load, 0)
    mixed[:, :, pl.ds(8, 8), :] = jnp.zeros((TILES, 2, 8, LANES), F32)
    mixed[:, :, pl.ds(144, 8), :] = jnp.zeros((TILES, 2, 8, LANES), F32)

    with jax.named_scope("load"):
        for tile in range(FIRST_COARSE_TILE, FIRST_COARSE_TILE + COARSE_TILES):
            wait_load(tile)

    def count(flag):
        return flag.astype(jnp.int32)

    with jax.named_scope("barrier"):
        own_kind = jnp.where(coarse, member + count(group > 0), 1 + count(place == 1))
        pl.semaphore_wait(barrier, 1 + count(rank > 0) + count(rank < space_size - 1) + own_kind)

    @pl.when(coarse)
    def _():
        @pl.when(group > 0)
        def _():
            pl.semaphore_signal(ready_carry, inc=1, device_id=facing(-1), device_id_type=MESH)

        def answer(index, carry):
            pl.semaphore_signal(ready, inc=1, device_id=in_group(index), device_id_type=MESH)
            return carry

        lax.fori_loop(0, member, answer, 0)

    parts = (pl.ds(FIRST_COARSE_TILE, COARSE_TILES), pl.ds(0, FIRST_COARSE_TILE),
             pl.ds(FIRST_COARSE_TILE + COARSE_TILES, TILES - FIRST_COARSE_TILE - COARSE_TILES))

    def halo(side, part):
        low, high = (ROWS, 0) if side == 0 else (8, ROWS + 8)
        return pltpu.make_async_remote_copy(
            src_ref=fields.at[parts[part], :, pl.ds(low, 8), :], dst_ref=fields.at[parts[part], :, pl.ds(high, 8), :],
            send_sem=halo_send.at[side, part], recv_sem=halo_recv.at[side, part],
            device_id={"tm": slot, "space": rank + 1 if side == 0 else rank - 1}, device_id_type=MESH)

    def send_halo(*which):
        @pl.when(rank < space_size - 1)
        def _():
            for part in which:
                halo(0, part).start()

        @pl.when(rank > 0)
        def _():
            for part in which:
                halo(1, part).start()

    def wait_halo(*which):
        @pl.when(rank > 0)
        def _():
            for part in which:
                halo(0, part).wait_recv()

        @pl.when(rank < space_size - 1)
        def _():
            for part in which:
                halo(1, part).wait_recv()

    send_halo(0)

    def bulk(rows, cols, index=0):
        return pltpu.make_async_remote_copy(
            src_ref=nodes_out.at[pl.ds(2, 2), rows, cols], dst_ref=next_out.at[:, rows, cols],
            send_sem=bulk_send.at[index], recv_sem=bulk_recv, device_id=at_slot(after), device_id_type=MESH)

    def push(rows, cols, index):
        @pl.when(slot < tm_size - 1)
        def _():
            bulk(rows, cols, index).start()

    def field(tile, plane, low, high):
        return fields[tile, plane, pl.ds(low + 8, high - low), :]

    def mix(tile, low, high):
        for part in range(2):
            mixed[tile, part, pl.ds(low + 16, high - low), :] = (
                (5.0 / 24.0) * field(tile, part, low, high) + (1.0 / 3.0) * field(tile, 2 + part, low, high)
                - (1.0 / 24.0) * field(tile, 4 + part, low, high))

    def beside(ref, lead, low, high):
        count = high - low
        real = ref[(*lead, 0, pl.ds(low + 15, count), slice(None))] + ref[(*lead, 0, pl.ds(low + 17, count), slice(None))]
        imag = ref[(*lead, 1, pl.ds(low + 15, count), slice(None))] + ref[(*lead, 1, pl.ds(low + 17, count), slice(None))]
        return real, imag

    def rates(tile, low, high):
        return rate_of(rank * ROWS + low, tile * LANES, high - low)

    def one(tile, low, high, scale=None, keep=False):
        rate_real, rate_imag, factor = rates(tile, low, high)
        inv_real, inv_imag = inverse(1.0 - 0.5 * rate_real, -0.5 * rate_imag)
        sum_real, sum_imag = beside(mixed, (tile,), low, high)
        begin = [field(tile, part, low, high) for part in range(2)]
        old_one = [field(tile, 2 + part, low, high) for part in range(2)]
        old_two = [field(tile, 4 + part, low, high) for part in range(2)]
        own = [(5.0 / 24.0) * begin[i] - (1.0 / 6.0) * old_one[i] - (1.0 / 24.0) * old_two[i] for i in range(2)]
        top = times(rate_real, rate_imag, *own)
        node = times(inv_real, inv_imag, begin[0] + top[0] + factor * sum_imag, begin[1] + top[1] - factor * sum_real)
        if scale is not None:
            node = [part * scale for part in node]
        for i in range(2):
            staged[tile, i, pl.ds(low + 16, high - low), :] = (
                (5.0 / 24.0) * old_two[i] - (1.0 / 24.0) * begin[i] - (1.0 / 6.0) * old_one[i] + 0.5 * node[i])
            if keep:
                node_one_buf[i, pl.ds(low + 16, high - low), :] = node[i]
            first, last = max(low, 0), min(high, ROWS)
            if first < last:
                nodes_out[i, pl.ds(first, last - first), columns(tile)] = node[i][first - low:last - low]

    def two(tile, low, high, keep=False):
        rate_real, rate_imag, factor = rates(tile, low, high)
        inv_real, inv_imag = inverse(1.0 - 0.5 * rate_real, -0.5 * rate_imag)
        sum_real, sum_imag = beside(staged, (tile,), low, high)
        begin = [field(tile, part, low, high) for part in range(2)]
        old_one = [field(tile, 2 + part, low, high) for part in range(2)]
        old_two = [field(tile, 4 + part, low, high) for part in range(2)]
        if keep:
            node = [node_one_buf[i, pl.ds(low + 16, high - low), :] for i in range(2)]
        else:
            node = [nodes_out[i, pl.ds(low, high - low), columns(tile)] for i in range(2)]
        own = [(1.0 / 3.0) * old_one[i] - (1.0 / 24.0) * begin[i] - (7.0 / 24.0) * old_two[i] for i in range(2)]
        top = times(rate_real, rate_imag, *own)
        last_node = times(inv_real, inv_imag, node[0] + top[0] + factor * sum_imag, node[1] + top[1] - factor * sum_real)
        for i in range(2):
            if keep:
                whole[i, pl.ds(low + 16, high - low), :] = (
                    (1.0 / 6.0) * begin[i] + (2.0 / 3.0) * node[i] + (1.0 / 6.0) * last_node[i])
            first, last = max(low, 0), min(high, ROWS)
            if first < last:
                nodes_out[2 + i, pl.ds(first, last - first), columns(tile)] = last_node[i][first - low:last - low]

    def inner(tile):
        for low in range(0, ROWS, 32):
            mix(tile, low, low + 32)
        for low in range(0, ROWS, 32):
            one(tile, low, low + 32)
        for low in (8, 40, 72, 104):
            two(tile, low, min(low + 32, 120))

    def rim(tile):
        mix(tile, -8, 0)
        mix(tile, ROWS, ROWS + 8)
        one(tile, -8, 8, scale=jnp.concatenate([jnp.full((8, LANES), (rank > 0).astype(F32)), jnp.ones((8, LANES), F32)]))
        one(tile, 120, 136,
            scale=jnp.concatenate([jnp.ones((8, LANES), F32), jnp.full((8, LANES), (rank < space_size - 1).astype(F32))]))
        two(tile, 0, 8)
        two(tile, 120, 128)

    middle = pl.ds(8, 112)
    upper = pl.ds(0, 8)
    lower = pl.ds(120, 8)

    def inner_push(index, carry):
        tile = tile_at(index)
        wait_load(tile)
        inner(tile)
        push(middle, columns(tile), index)
        return carry

    def edge(index, carry):
        rim(tile_at(index))
        return carry

    def settle(cols):
        @pl.when(slot > 0)
        def _():
            bulk(slice(None), cols).wait_recv()

    @pl.when(fine)
    def _():
        def relay_source(chunk):
            rows = pl.ds(pl.multiple_of(8 + lax.rem(chunk, 2) * RELAY_ROWS, 8), RELAY_ROWS)
            return rows, columns(tile_at(LEAD + chunk // 2))

        def leg(which, chunk):
            rows, cols = relay_source(chunk)
            if which == 0:
                source, target, device = nodes_out.at[pl.ds(2, 2), rows, cols], first_leg.at[chunk], at_slot(below)
                recv = relay_recv.at[0, chunk]
            elif which == 1:
                source, target, device, recv = first_leg.at[chunk], second_leg.at[chunk], at_slot(below), relay_recv.at[1, chunk]
            else:
                origin = column * RING + lax.rem(place + 2, RING)
                source, target, device, recv = second_leg.at[chunk], next_out.at[:, rows, cols], at_slot(origin + 1), bulk_recv
            return pltpu.make_async_remote_copy(
                src_ref=source, dst_ref=target, send_sem=relay_send.at[which, chunk], recv_sem=recv,
                device_id=device, device_id_type=MESH)

        def relayed(which):
            start = lax.rem(place + which, RING)
            wraps = (start == RING - 1).astype(jnp.int32)
            return 2 + RELAY_WRAP * wraps + count(shared) * (RELAY_SHARED + RELAY_BOTH * wraps)

        def has_origin(which):
            return column * RING + lax.rem(place + which, RING) < tm_size - 1

        def aside_tile(index):
            return (index >= LEAD) & (index < LEAD + relayed(0))

        def start_tile(index, carry):
            @pl.when(index >= COARSE_TILES)
            def _():
                wait_load(tile_at(index))

            inner(tile_at(index))

            @pl.when(has_origin(0) & aside_tile(index))
            def _():
                leg(0, 2 * (index - LEAD)).start()
                leg(0, 2 * (index - LEAD) + 1).start()

            @pl.when(has_origin(0) & jnp.logical_not(aside_tile(index)))
            def _():
                bulk(middle, columns(tile_at(index)), index).start()

            return carry

        def forward(which, chunk):
            @pl.when(has_origin(which) & (chunk < 2 * relayed(which)))
            def _():
                leg(which - 1, chunk).wait_recv()
                leg(which, chunk).start()

        with jax.named_scope("inner"):
            lax.fori_loop(0, TILES, start_tile, 0)
        send_halo(1, 2)
        with jax.named_scope("fwdA"):
            forward(1, 0)
            forward(1, 1)
        with jax.named_scope("halo"):
            wait_halo(0, 1, 2)

        @pl.when(rank == 0)
        def _():
            fields[:, :, pl.ds(0, 8), :] = jnp.zeros((TILES, 6, 8, LANES), F32)

        @pl.when(rank == space_size - 1)
        def _():
            fields[:, :, pl.ds(ROWS + 8, 8), :] = jnp.zeros((TILES, 6, 8, LANES), F32)

        with jax.named_scope("rim"):
            lax.fori_loop(0, TILES, edge, 0)
        push(upper, slice(None), TILES)
        push(lower, slice(None), TILES + 1)

        def pass_on(step, carry):
            forward(1, step)
            forward(2, step - 2)
            return carry

        with jax.named_scope("fwdB"):
            lax.fori_loop(2, RELAYS + 2, pass_on, 0)
        with jax.named_scope("settle"):
            settle(slice(None))

        @pl.when(slot < tm_size - 1)
        def _():
            def sent(index, carry):
                @pl.when(jnp.logical_not(aside_tile(index)))
                def _():
                    bulk(middle, columns(tile_at(index)), index).wait_send()

                return carry

            lax.fori_loop(0, TILES, sent, 0)
            bulk(upper, slice(None), TILES).wait_send()
            bulk(lower, slice(None), TILES + 1).wait_send()

        for which in range(3):
            def legs_sent(chunk, carry):
                @pl.when(has_origin(which) & (chunk < 2 * relayed(which)))
                def _():
                    leg(which, chunk).wait_send()

                return carry

            lax.fori_loop(0, RELAYS, legs_sent, 0)

    @pl.when(coarse)
    def _():
        lead = (slot == 0).astype(F32)

        def piece(index):
            row = index // RING
            number = jnp.where(lax.rem(group, 2) == 1, depth - 1 - row, row) * RING + lax.rem(index, RING)
            share = GROUP // COARSE_TILES
            rows = pl.ds(pl.multiple_of(lax.rem(number, share) * PIECE_ROWS, 8), PIECE_ROWS)
            return number // share, slice(None), rows, slice(None)

        def push_only(index, carry):
            push(middle, columns(tile_at(index)), index)
            return carry

        lax.fori_loop(COARSE_TILES, TILES, lambda index, carry: (wait_load(tile_at(index)), carry)[1], 0)
        send_halo(1, 2)
        with jax.named_scope("innerA"):
            def inner_and_push(index, carry):
                inner(tile_at(index))

                @pl.when(index < first_pushes)
                def _():
                    push_only(index, 0)

                return carry

            first_pushes = COARSE_TILES + jnp.where(place == RING - 1, FIRST_WRAP, FIRST)
            lax.fori_loop(COARSE_TILES, TILES, inner_and_push, 0)
        with jax.named_scope("halo"):
            wait_halo(0)

        def full(tile, carry):
            bands = ((-8, 24), (24, 56), (56, 88), (88, 120), (120, 136))
            for low, high in bands:
                mix(tile, low, high)
            for low, high in bands:
                one(tile, low, high, keep=True)
            for low, high in bands:
                two(tile, low, high, keep=True)
            for low in range(0, ROWS, 32):
                rate_real, rate_imag, factor = rates(tile, low, low + 32)
                sum_real, sum_imag = beside(whole, (), low, low + 32)
                own = [whole[i, pl.ds(low + 16, 32), :] - nodes_out[2 + i, pl.ds(low, 32), columns(tile)] for i in range(2)]
                top = times(rate_real, rate_imag, *own)
                offset[tile - FIRST_COARSE_TILE, 0, pl.ds(low, 32), :] = top[0] + factor * sum_imag + lead * field(tile, 0, low, low + 32)
                offset[tile - FIRST_COARSE_TILE, 1, pl.ds(low, 32), :] = top[1] - factor * sum_real + lead * field(tile, 1, low, low + 32)
            return carry

        def gather(source, target):
            return pltpu.make_async_remote_copy(
                src_ref=offset.at[piece(target)], dst_ref=gathered.at[source], send_sem=gather_send.at[target],
                recv_sem=gather_recv.at[source], device_id=in_group(target), device_id_type=MESH)

        def scatter(source, target):
            return pltpu.make_async_remote_copy(
                src_ref=results.at[target], dst_ref=begins.at[piece(source)], send_sem=scatter_send.at[target],
                recv_sem=scatter_recv.at[source], device_id=in_group(target), device_id_type=MESH)

        def hand_on():
            return pltpu.make_async_remote_copy(
                src_ref=carry_out, dst_ref=carry_in, send_sem=carry_send, recv_sem=carry_recv, device_id=facing(1),
                device_id_type=MESH)

        row = member // RING
        beside_row = (row + 1 - 2 * lax.rem(row, 2)) * RING

        def detour(stage):
            source = offset.at[piece(row * RING)] if stage == 0 else results.at[row * RING]
            sem = gather_send if stage == 0 else scatter_send
            return pltpu.make_async_remote_copy(
                src_ref=source, dst_ref=aside.at[stage], send_sem=sem.at[row * RING], recv_sem=aside_recv.at[stage],
                device_id=in_group(beside_row), device_id_type=MESH)

        def relay_aside(stage):
            origin = beside_row + RING - 1
            target = gathered.at[origin] if stage == 0 else begins.at[piece(origin)]
            sem = gather_recv if stage == 0 else scatter_recv
            return pltpu.make_async_remote_copy(
                src_ref=aside.at[stage], dst_ref=target, send_sem=aside_send.at[stage], recv_sem=sem.at[origin],
                device_id=in_group(beside_row), device_id_type=MESH)

        def crowded(stage):
            return group >= 0 if stage == 0 else group < ASIDE_GROUPS

        def pass_aside(stage):
            @pl.when((place == 0) & crowded(stage))
            def _():
                detour(stage).wait_recv()
                relay_aside(stage).start()

        def blocked(target, stage):
            return (place == RING - 1) & (target == row * RING) & crowded(stage)

        def other(distance):
            return lax.rem(member + distance, GROUP)

        with jax.named_scope("full"):
            lax.fori_loop(FIRST_COARSE_TILE, FIRST_COARSE_TILE + COARSE_TILES, full, 0)
        with jax.named_scope("ready"):
            @pl.when(member < GROUP - 1)
            def _():
                pl.semaphore_wait(ready, GROUP - 1 - member)

        def spread(distance, carry):
            @pl.when(jnp.logical_not(blocked(other(distance), 0)))
            def _():
                gather(member, other(distance)).start()

            return carry

        with jax.named_scope("spread"):
            @pl.when(place == RING - 1)
            def _():
                detour(0).start()

            lax.fori_loop(1, GROUP, spread, 0)
        gathered[member] = offset[piece(member)]
        early = jnp.where(place == RING - 1, EARLY_WRAP + group * WRAP_STEP // 2, EARLY + group * EARLY_STEP // 2)
        early = jnp.minimum(early, TILES)
        early = jnp.maximum(early, first_pushes)
        lax.fori_loop(first_pushes, early, push_only, 0)
        with jax.named_scope("halo2"):
            wait_halo(1, 2)
        with jax.named_scope("rim"):
            lax.fori_loop(COARSE_TILES, TILES, edge, 0)
        tile, _, _, _ = piece(member)
        number = jnp.where(lax.rem(group, 2) == 1, depth - 1 - member // RING, member // RING) * RING + place
        first = lax.rem(number, GROUP // COARSE_TILES) * PIECE_ROWS
        rate_real, rate_imag, _ = rate_of(rank * ROWS + first, (FIRST_COARSE_TILE + tile) * LANES, PIECE_ROWS)
        gain = inverse(1.0 - rate_real, -rate_imag)

        with jax.named_scope("aside0"):
            pass_aside(0)
        with jax.named_scope("gather"):
            def arrive(distance, carry):
                gather(other(distance), member).wait_recv()
                return carry

            lax.fori_loop(1, GROUP, arrive, 0)

        with jax.named_scope("carry"):
            @pl.when(group == 0)
            def _():
                carry_in[...] = jnp.zeros((2, PIECE_ROWS, LANES), F32)

            @pl.when(group > 0)
            def _():
                hand_on().wait_recv()

        def scan(index, running):
            for i in range(2):
                results[index, i] = running[i]
            return times(*gain, running[0] + gathered[index, 0], running[1] + gathered[index, 1])

        with jax.named_scope("scan"):
            running = lax.fori_loop(0, GROUP, scan, (carry_in[0], carry_in[1]))
            for i in range(2):
                carry_out[i] = running[i]

            @pl.when(group < groups - 1)
            def _():
                pl.semaphore_wait(ready_carry, 1)
                hand_on().start()

        def give(distance, carry):
            @pl.when(jnp.logical_not(blocked(other(distance), 1)))
            def _():
                scatter(member, other(distance)).start()

            return carry

        with jax.named_scope("give"):
            @pl.when((place == RING - 1) & crowded(1))
            def _():
                detour(1).start()

            lax.fori_loop(1, GROUP, give, 0)
        begins[piece(member)] = results[member]
        lax.fori_loop(early, TILES, push_only, 0)
        left = pl.ds(0, FIRST_COARSE_TILE * LANES)
        right_start = (FIRST_COARSE_TILE + COARSE_TILES) * LANES
        right = pl.ds(right_start, KY - right_start)
        rims = [(upper, left), (upper, right), (lower, left), (lower, right)]
        for number, (rows, cols) in enumerate(rims):
            push(rows, cols, TILES + number)

        with jax.named_scope("aside1"):
            pass_aside(1)
        with jax.named_scope("back"):
            def fetch(distance, carry):
                scatter(other(distance), member).wait_recv()
                return carry

            lax.fori_loop(1, GROUP, fetch, 0)

        later = 1.0 - lead

        def finish(tile, carry):
            which = tile - FIRST_COARSE_TILE
            for low in range(0, ROWS, 32):
                rows = pl.ds(low, 32)
                rate_real, rate_imag, _ = rates(tile, low, low + 32)
                inv_real, inv_imag = inverse(1.0 - rate_real, -rate_imag)
                begin_new = [begins[which, i, rows, :] for i in range(2)]
                end_new = times(inv_real, inv_imag, *[begin_new[i] + offset[which, i, rows, :] for i in range(2)])
                for i in range(2):
                    old_end = nodes_out[2 + i, rows, columns(tile)]
                    nodes_out[i, rows, columns(tile)] += 0.5 * (
                        (begin_new[i] - later * field(tile, i, low, low + 32)) + (end_new[i] - old_end))
                    nodes_out[2 + i, rows, columns(tile)] = end_new[i]
                    next_out[i, rows, columns(tile)] = begin_new[i]
            return carry

        with jax.named_scope("finish"):
            lax.fori_loop(FIRST_COARSE_TILE, FIRST_COARSE_TILE + COARSE_TILES, finish, 0)

        with jax.named_scope("settle"):
            settle(pl.ds(0, FINE_TILES * LANES))

        @pl.when(slot < tm_size - 1)
        def _():
            def sent(index, carry):
                bulk(middle, columns(tile_at(index)), index).wait_send()
                return carry

            lax.fori_loop(COARSE_TILES, TILES, sent, 0)
            for number, (rows, cols) in enumerate(rims):
                bulk(rows, cols, TILES + number).wait_send()

        @pl.when(group < groups - 1)
        def _():
            hand_on().wait_send()

        def let_go(distance, carry):
            gather(member, other(distance)).wait_send()
            scatter(member, other(distance)).wait_send()
            return carry

        lax.fori_loop(1, GROUP, let_go, 0)

        for stage in range(2):
            @pl.when((place == 0) & crowded(stage))
            def _():
                relay_aside(stage).wait_send()

    @pl.when(rank < space_size - 1)
    def _():
        for part in range(3):
            halo(0, part).wait_send()

    @pl.when(rank > 0)
    def _():
        for part in range(3):
            halo(1, part).wait_send()

    @pl.when(slot == 0)
    def _():
        def restore(tile, carry):
            for i in range(2):
                next_out[i, :, columns(tile)] = fields[tile, i, pl.ds(8, ROWS), :]
            return carry

        lax.fori_loop(0, TILES, restore, 0)


def deliver(start_ref, nodes_ref, start_hbm, nodes_hbm, sems):
    copies = [pltpu.make_async_copy(nodes_ref.at[i], nodes_hbm.at[i], sems.at[i]) for i in range(4)]
    copies += [pltpu.make_async_copy(start_ref.at[i], start_hbm.at[i], sems.at[4 + i]) for i in range(2)]
    for copy in copies:
        copy.start()
    for copy in copies:
        copy.wait()


def solution(mesh):
    tm_size, space_size = mesh.shape["tm"], mesh.shape["space"]

    def body(start_values, node_values):
        hbm = pl.BlockSpec(memory_space=pltpu.MemorySpace.HBM)
        vmem = pl.BlockSpec(memory_space=pltpu.MemorySpace.VMEM)
        dma = pltpu.SemaphoreType.DMA
        next_start, nodes = pl.pallas_call(
            functools.partial(kernel, tm_size, space_size),
            out_shape=(pltpu.MemorySpace.VMEM((2, ROWS, KY), F32), pltpu.MemorySpace.VMEM((4, ROWS, KY), F32)),
            in_specs=[hbm, hbm],
            out_specs=(vmem, vmem),
            scratch_shapes=[
                pltpu.VMEM((TILES, 6, ROWS + 16, LANES), F32),
                pltpu.VMEM((TILES, 2, ROWS + 32, LANES), F32),
                pltpu.VMEM((TILES, 2, ROWS + 32, LANES), F32),
                pltpu.VMEM((2, ROWS + 32, LANES), F32),
                pltpu.VMEM((2, ROWS + 32, LANES), F32),
                pltpu.VMEM((COARSE_TILES, 2, ROWS, LANES), F32),
                pltpu.VMEM((GROUP, 2, PIECE_ROWS, LANES), F32),
                pltpu.VMEM((2, PIECE_ROWS, LANES), F32),
                pltpu.VMEM((2, PIECE_ROWS, LANES), F32),
                pltpu.VMEM((GROUP, 2, PIECE_ROWS, LANES), F32),
                pltpu.VMEM((COARSE_TILES, 2, ROWS, LANES), F32),
                pltpu.VMEM((RELAYS, 2, RELAY_ROWS, LANES), F32),
                pltpu.VMEM((RELAYS, 2, RELAY_ROWS, LANES), F32),
                dma((TILES, 2)),
                dma((2, 3)),
                dma((2, 3)),
                dma((TILES + 4,)),
                dma,
                dma((GROUP,)),
                dma((GROUP,)),
                dma,
                dma,
                dma((GROUP,)),
                dma((GROUP,)),
                dma((3, RELAYS)),
                dma((2, RELAYS)),
                pltpu.SemaphoreType.REGULAR,
                pltpu.SemaphoreType.REGULAR,
                pltpu.VMEM((2, 2, PIECE_ROWS, LANES), F32),
                dma((2,)),
                dma((2,)),
            ],
            compiler_params=pltpu.CompilerParams(collective_id=0, has_side_effects=True, vmem_limit_bytes=61696 * 1024),
            name="pfasst",
        )(start_values[0], node_values[0].reshape(4, ROWS, KY))
        next_start, nodes = pl.pallas_call(
            deliver,
            out_shape=(jax.ShapeDtypeStruct((2, ROWS, KY), F32), jax.ShapeDtypeStruct((4, ROWS, KY), F32)),
            in_specs=[vmem, vmem],
            out_specs=(hbm, hbm),
            scratch_shapes=[dma((6,))],
            compiler_params=pltpu.CompilerParams(vmem_limit_bytes=2**20),
            name="deliver",
        )(next_start, nodes)
        return next_start[None], nodes.reshape(1, 2, 2, ROWS, KY)

    return jax.shard_map(
        body,
        mesh=mesh,
        in_specs=(P("tm", None, "space", None), P("tm", None, None, "space", None)),
        out_specs=(P("tm", None, "space", None), P("tm", None, None, "space", None)),
        check_vma=False,
    )
```

```python
import functools

import jax
import jax.numpy as jnp
from jax import lax
from jax.experimental import pallas as pl
from jax.experimental.pallas import tpu as pltpu
from jax.sharding import PartitionSpec as P

MESH = pl.DeviceIdType.MESH
F32 = jnp.float32
KX = 1024
KY = 1024
CX = 256
LANES = 128
ROWS = 128
TILES = KY // LANES
FIRST_COARSE_TILE = (KY // 2 - CX // 2) // LANES
COARSE_TILES = CX // LANES
FIRST_COARSE_RANK = (KX // 2 - CX // 2) // ROWS
COARSE_RANKS = CX // ROWS
FINE_TILES = TILES - COARSE_TILES
RING = 4
GROUP = 8
PIECE_ROWS = COARSE_TILES * ROWS // GROUP
RELAY_SHARED = 1
RELAY_WRAP = 1
RELAY_BOTH = 1
RELAYS = 2 * (2 + RELAY_SHARED + RELAY_WRAP + RELAY_BOTH)
RELAY_ROWS = 56
EARLY = 4
EARLY_WRAP = 5
EARLY_STEP = 2
WRAP_STEP = 2
LEAD = 1
EARLY_ZERO = 2
LAG = 6
ASIDE_GROUPS = 2
FIRST = 2
FIRST_WRAP = 2

diffusion = 1.5
drift = 0.8
shear = 0.6


def columns(tile):
    return pl.ds(pl.multiple_of(tile * LANES, LANES), LANES)


def rate_of(first_row, first_column, rows):
    row = (first_row + lax.broadcasted_iota(jnp.int32, (rows, LANES), 0)).astype(F32)
    column = (first_column + lax.broadcasted_iota(jnp.int32, (rows, LANES), 1)).astype(F32)
    along = (row - KX // 2) / (KX // 2)
    across = (column - KY // 2) / (KY // 2)
    return -diffusion * (along * along + across * across), -drift * across, shear * across


def times(ar, ai, br, bi):
    return ar * br - ai * bi, ar * bi + ai * br


def inverse(real_part, imag_part):
    scale = 1.0 / (real_part * real_part + imag_part * imag_part)
    return real_part * scale, -imag_part * scale


def tile_at(index):
    early = jnp.where(index < COARSE_TILES, index + FIRST_COARSE_TILE, index - COARSE_TILES)
    return jnp.where(index < FIRST_COARSE_TILE + COARSE_TILES, early, index)


def kernel(tm_size, space_size, start_hbm, nodes_hbm, next_out, nodes_out, fields, mixed, staged, node_one_buf, whole, offset,
           gathered, prefix, carry_in, carry_out, results, begins, first_leg, second_leg, load_sem, halo_send, halo_recv, bulk_send,
           bulk_recv, gather_send, gather_recv, carry_send, carry_recv, scatter_send, scatter_recv, relay_send, relay_recv,
           ready, ready_carry, aside, aside_send, aside_recv):
    slot = lax.axis_index("tm")
    rank = lax.axis_index("space")
    coarse = (rank >= FIRST_COARSE_RANK) & (rank < FIRST_COARSE_RANK + COARSE_RANKS)
    fine = jnp.logical_not(coarse)
    shared = (rank == FIRST_COARSE_RANK - 1) | (rank == FIRST_COARSE_RANK + COARSE_RANKS)
    column, place = slot // RING, lax.rem(slot, RING)

    def at_slot(index):
        return {"tm": lax.rem(index, tm_size), "space": rank}

    after = slot + 1
    before = slot + tm_size - 1
    above = column * RING + lax.rem(place + 1, RING)
    below = column * RING + lax.rem(place + RING - 1, RING)

    def loads(tile):
        body = pl.ds(8, ROWS)
        return (
            pltpu.make_async_copy(start_hbm.at[:, :, columns(tile)], fields.at[tile, pl.ds(0, 2), body, :], load_sem.at[tile]),
            pltpu.make_async_copy(nodes_hbm.at[:, :, columns(tile)], fields.at[tile, pl.ds(2, 4), body, :], load_sem.at[tile]),
        )

    def wait_load(tile):
        landed = fields.at[tile, :, pl.ds(8, ROWS), :]
        pltpu.make_async_copy(landed, landed, load_sem.at[tile]).wait()

    barrier = pltpu.get_barrier_semaphore()

    def greet(target):
        pl.semaphore_signal(barrier, inc=1, device_id=target, device_id_type=MESH)

    @pl.when(rank > 0)
    def _():
        greet({"tm": slot, "space": rank - 1})

    @pl.when(rank < space_size - 1)
    def _():
        greet({"tm": slot, "space": rank + 1})

    greet(at_slot(before))

    @pl.when(fine)
    def _():
        greet(at_slot(above))

        @pl.when(place == 0)
        def _():
            greet(at_slot(slot + tm_size - RING + 1))

    member, group = lax.rem(slot, GROUP), slot // GROUP
    groups = tm_size // GROUP
    def in_group(index):
        return at_slot(group * GROUP + index)

    def facing(index):
        return at_slot(index * GROUP + member)

    @pl.when(coarse)
    def _():
        def call(index, carry):
            greet(in_group(index))
            return carry

        lax.fori_loop(member + 1, GROUP, call, 0)

        def call_later(index, carry):
            greet(facing(index))
            return carry

        lax.fori_loop(group + 1, groups, call_later, 0)

    def begin_load(index, carry):
        for copy in loads(tile_at(index)):
            copy.start()
        return carry

    lax.fori_loop(0, TILES, begin_load, 0)
    mixed[:, :, pl.ds(8, 8), :] = jnp.zeros((TILES, 2, 8, LANES), F32)
    mixed[:, :, pl.ds(144, 8), :] = jnp.zeros((TILES, 2, 8, LANES), F32)

    with jax.named_scope("load"):
        for tile in range(FIRST_COARSE_TILE, FIRST_COARSE_TILE + COARSE_TILES):
            wait_load(tile)

    def count(flag):
        return flag.astype(jnp.int32)

    with jax.named_scope("barrier"):
        own_kind = jnp.where(coarse, member + group, 1 + count(place == 1))
        pl.semaphore_wait(barrier, 1 + count(rank > 0) + count(rank < space_size - 1) + own_kind)

    @pl.when(coarse)
    def _():
        def answer_earlier(index, carry):
            pl.semaphore_signal(ready_carry, inc=1, device_id=facing(index), device_id_type=MESH)
            return carry

        lax.fori_loop(0, group, answer_earlier, 0)

        def answer(index, carry):
            pl.semaphore_signal(ready, inc=1, device_id=in_group(index), device_id_type=MESH)
            return carry

        lax.fori_loop(0, member, answer, 0)

    parts = (pl.ds(FIRST_COARSE_TILE, COARSE_TILES), pl.ds(0, FIRST_COARSE_TILE),
             pl.ds(FIRST_COARSE_TILE + COARSE_TILES, TILES - FIRST_COARSE_TILE - COARSE_TILES))

    def halo(side, part):
        low, high = (ROWS, 0) if side == 0 else (8, ROWS + 8)
        return pltpu.make_async_remote_copy(
            src_ref=fields.at[parts[part], :, pl.ds(low, 8), :], dst_ref=fields.at[parts[part], :, pl.ds(high, 8), :],
            send_sem=halo_send.at[side], recv_sem=halo_recv.at[side, part],
            device_id={"tm": slot, "space": rank + 1 if side == 0 else rank - 1}, device_id_type=MESH)

    def send_halo(*which):
        @pl.when(rank < space_size - 1)
        def _():
            for part in which:
                halo(0, part).start()

        @pl.when(rank > 0)
        def _():
            for part in which:
                halo(1, part).start()

    def wait_halo(*which):
        @pl.when(rank > 0)
        def _():
            for part in which:
                halo(0, part).wait_recv()

        @pl.when(rank < space_size - 1)
        def _():
            for part in which:
                halo(1, part).wait_recv()

    def all_of(ref, send, recv):
        return pltpu.make_async_remote_copy(
            src_ref=ref, dst_ref=ref, send_sem=send, recv_sem=recv, device_id=at_slot(after), device_id_type=MESH)

    def halo_sent():
        edge_rows = fields.at[:, :, pl.ds(0, 8), :]

        @pl.when(rank < space_size - 1)
        def _():
            all_of(edge_rows, halo_send.at[0], halo_recv.at[0, 0]).wait_send()

        @pl.when(rank > 0)
        def _():
            all_of(edge_rows, halo_send.at[1], halo_recv.at[0, 0]).wait_send()

    send_halo(0)

    def bulk(rows, cols, index=0):
        return pltpu.make_async_remote_copy(
            src_ref=nodes_out.at[pl.ds(2, 2), rows, cols], dst_ref=next_out.at[:, rows, cols],
            send_sem=bulk_send.at[index], recv_sem=bulk_recv, device_id=at_slot(after), device_id_type=MESH)

    def push(rows, cols, index=0):
        @pl.when(slot < tm_size - 1)
        def _():
            bulk(rows, cols, index).start()

    def field(tile, plane, low, high):
        return fields[tile, plane, pl.ds(low + 8, high - low), :]

    def mix(tile, low, high):
        for part in range(2):
            mixed[tile, part, pl.ds(low + 16, high - low), :] = (
                (5.0 / 24.0) * field(tile, part, low, high) + (1.0 / 3.0) * field(tile, 2 + part, low, high)
                - (1.0 / 24.0) * field(tile, 4 + part, low, high))

    def beside(ref, lead, low, high):
        count = high - low
        real = ref[(*lead, 0, pl.ds(low + 15, count), slice(None))] + ref[(*lead, 0, pl.ds(low + 17, count), slice(None))]
        imag = ref[(*lead, 1, pl.ds(low + 15, count), slice(None))] + ref[(*lead, 1, pl.ds(low + 17, count), slice(None))]
        return real, imag

    def rates(tile, low, high):
        return rate_of(rank * ROWS + low, tile * LANES, high - low)

    def one(tile, low, high, scale=None, keep=False):
        rate_real, rate_imag, factor = rates(tile, low, high)
        inv_real, inv_imag = inverse(1.0 - 0.5 * rate_real, -0.5 * rate_imag)
        sum_real, sum_imag = beside(mixed, (tile,), low, high)
        begin = [field(tile, part, low, high) for part in range(2)]
        old_one = [field(tile, 2 + part, low, high) for part in range(2)]
        old_two = [field(tile, 4 + part, low, high) for part in range(2)]
        own = [(5.0 / 24.0) * begin[i] - (1.0 / 6.0) * old_one[i] - (1.0 / 24.0) * old_two[i] for i in range(2)]
        top = times(rate_real, rate_imag, *own)
        node = times(inv_real, inv_imag, begin[0] + top[0] + factor * sum_imag, begin[1] + top[1] - factor * sum_real)
        if scale is not None:
            node = [part * scale for part in node]
        for i in range(2):
            staged[tile, i, pl.ds(low + 16, high - low), :] = (
                (5.0 / 24.0) * old_two[i] - (1.0 / 24.0) * begin[i] - (1.0 / 6.0) * old_one[i] + 0.5 * node[i])
            if keep:
                node_one_buf[i, pl.ds(low + 16, high - low), :] = node[i]
            first, last = max(low, 0), min(high, ROWS)
            if first < last:
                nodes_out[i, pl.ds(first, last - first), columns(tile)] = node[i][first - low:last - low]

    def two(tile, low, high, keep=False):
        rate_real, rate_imag, factor = rates(tile, low, high)
        inv_real, inv_imag = inverse(1.0 - 0.5 * rate_real, -0.5 * rate_imag)
        sum_real, sum_imag = beside(staged, (tile,), low, high)
        begin = [field(tile, part, low, high) for part in range(2)]
        old_one = [field(tile, 2 + part, low, high) for part in range(2)]
        old_two = [field(tile, 4 + part, low, high) for part in range(2)]
        if keep:
            node = [node_one_buf[i, pl.ds(low + 16, high - low), :] for i in range(2)]
        else:
            node = [nodes_out[i, pl.ds(low, high - low), columns(tile)] for i in range(2)]
        own = [(1.0 / 3.0) * old_one[i] - (1.0 / 24.0) * begin[i] - (7.0 / 24.0) * old_two[i] for i in range(2)]
        top = times(rate_real, rate_imag, *own)
        last_node = times(inv_real, inv_imag, node[0] + top[0] + factor * sum_imag, node[1] + top[1] - factor * sum_real)
        for i in range(2):
            if keep:
                whole[i, pl.ds(low + 16, high - low), :] = (
                    (1.0 / 6.0) * begin[i] + (2.0 / 3.0) * node[i] + (1.0 / 6.0) * last_node[i])
            first, last = max(low, 0), min(high, ROWS)
            if first < last:
                nodes_out[2 + i, pl.ds(first, last - first), columns(tile)] = last_node[i][first - low:last - low]

    def inner(tile):
        for low in range(0, ROWS, 32):
            mix(tile, low, low + 32)
        for low in range(0, ROWS, 32):
            one(tile, low, low + 32)
        for low in (8, 40, 72, 104):
            two(tile, low, min(low + 32, 120))

    def rim(tile):
        mix(tile, -8, 0)
        mix(tile, ROWS, ROWS + 8)
        one(tile, -8, 8, scale=jnp.concatenate([jnp.full((8, LANES), (rank > 0).astype(F32)), jnp.ones((8, LANES), F32)]))
        one(tile, 120, 136,
            scale=jnp.concatenate([jnp.ones((8, LANES), F32), jnp.full((8, LANES), (rank < space_size - 1).astype(F32))]))
        two(tile, 0, 8)
        two(tile, 120, 128)

    middle = pl.ds(8, 112)
    upper = pl.ds(0, 8)
    lower = pl.ds(120, 8)

    def edge(index, carry):
        rim(tile_at(index))
        return carry

    def settle(cols):
        @pl.when(slot > 0)
        def _():
            bulk(slice(None), cols).wait_recv()

    @pl.when(fine)
    def _():
        def relay_source(chunk):
            rows = pl.ds(pl.multiple_of(8 + lax.rem(chunk, 2) * RELAY_ROWS, 8), RELAY_ROWS)
            return rows, columns(tile_at(LEAD + chunk // 2))

        def leg(which, chunk):
            rows, cols = relay_source(chunk)
            if which == 0:
                source, target, device = nodes_out.at[pl.ds(2, 2), rows, cols], first_leg.at[chunk], at_slot(below)
                recv = relay_recv.at[0, chunk]
            elif which == 1:
                source, target, device, recv = first_leg.at[chunk], second_leg.at[chunk], at_slot(below), relay_recv.at[1, chunk]
            else:
                origin = column * RING + lax.rem(place + 2, RING)
                source, target, device, recv = second_leg.at[chunk], next_out.at[:, rows, cols], at_slot(origin + 1), bulk_recv
            return pltpu.make_async_remote_copy(
                src_ref=source, dst_ref=target, send_sem=relay_send.at[which], recv_sem=recv,
                device_id=device, device_id_type=MESH)

        def relayed(which):
            start = lax.rem(place + which, RING)
            wraps = (start == RING - 1).astype(jnp.int32)
            return 2 + RELAY_WRAP * wraps + count(shared) * (RELAY_SHARED + RELAY_BOTH * wraps)

        def has_origin(which):
            return column * RING + lax.rem(place + which, RING) < tm_size - 1

        def aside_tile(index):
            return (index >= LEAD) & (index < LEAD + relayed(0))

        def start_tile(index, carry):
            @pl.when(index >= COARSE_TILES)
            def _():
                wait_load(tile_at(index))

            inner(tile_at(index))

            @pl.when(has_origin(0) & aside_tile(index))
            def _():
                leg(0, 2 * (index - LEAD)).start()
                leg(0, 2 * (index - LEAD) + 1).start()

            @pl.when(has_origin(0) & jnp.logical_not(aside_tile(index)))
            def _():
                bulk(middle, columns(tile_at(index))).start()

            return carry

        def forward(which, chunk):
            @pl.when(has_origin(which) & (chunk >= 0) & (chunk < 2 * relayed(which)))
            def _():
                leg(which - 1, chunk).wait_recv()
                leg(which, chunk).start()

        with jax.named_scope("inner"):
            lax.fori_loop(0, TILES, start_tile, 0)
        send_halo(1, 2)
        with jax.named_scope("fwdA"):
            forward(1, 0)
            forward(1, 1)
        with jax.named_scope("halo"):
            wait_halo(0, 1, 2)

        @pl.when(rank == 0)
        def _():
            fields[:, :, pl.ds(0, 8), :] = jnp.zeros((TILES, 6, 8, LANES), F32)

        @pl.when(rank == space_size - 1)
        def _():
            fields[:, :, pl.ds(ROWS + 8, 8), :] = jnp.zeros((TILES, 6, 8, LANES), F32)

        with jax.named_scope("rim"):
            lax.fori_loop(0, TILES, edge, 0)
        push(upper, slice(None), 1)
        push(lower, slice(None), 1)

        def pass_on(step, carry):
            forward(1, step)
            forward(2, step - LAG)
            return carry

        with jax.named_scope("fwdB"):
            lax.fori_loop(2, RELAYS + LAG, pass_on, 0)
        halo_sent()

        def tiles_sent(relays):
            return bulk(middle, pl.ds(0, (TILES - relays) * LANES)), first_leg.at[pl.ds(0, 2 * relays)]

        for relays in range(2, RELAYS // 2 + 1):
            direct, chunks = tiles_sent(relays)
            for which in range(3):
                @pl.when(has_origin(which) & (relayed(which) == relays))
                def _():
                    all_of(chunks, relay_send.at[which], relay_recv.at[0, 0]).wait_send()

            @pl.when(has_origin(0) & (relayed(0) == relays))
            def _():
                direct.wait_send()

        @pl.when(has_origin(0))
        def _():
            bulk(pl.ds(0, 16), slice(None), 1).wait_send()

        with jax.named_scope("settle"):
            settle(slice(None))

    @pl.when(coarse)
    def _():
        lead = (slot == 0).astype(F32)

        def piece(index):
            share = GROUP // COARSE_TILES
            rows = pl.ds(pl.multiple_of(lax.rem(index, share) * PIECE_ROWS, 8), PIECE_ROWS)
            return index // share, slice(None), rows, slice(None)

        def push_only(index, carry):
            push(middle, columns(tile_at(index)))
            return carry

        lax.fori_loop(COARSE_TILES, TILES, lambda index, carry: (wait_load(tile_at(index)), carry)[1], 0)
        send_halo(1, 2)
        with jax.named_scope("innerA"):
            def inner_and_push(index, carry):
                inner(tile_at(index))

                @pl.when(index < first_pushes)
                def _():
                    push_only(index, 0)

                return carry

            first_pushes = COARSE_TILES + jnp.where(place == RING - 1, FIRST_WRAP, FIRST)
            lax.fori_loop(COARSE_TILES, TILES, inner_and_push, 0)
        with jax.named_scope("halo"):
            wait_halo(0)

        def full(tile, carry):
            bands = ((-8, 24), (24, 56), (56, 88), (88, 120), (120, 136))
            for low, high in bands:
                mix(tile, low, high)
            for low, high in bands:
                one(tile, low, high, keep=True)
            for low, high in bands:
                two(tile, low, high, keep=True)
            for low in range(0, ROWS, 32):
                rate_real, rate_imag, factor = rates(tile, low, low + 32)
                sum_real, sum_imag = beside(whole, (), low, low + 32)
                own = [whole[i, pl.ds(low + 16, 32), :] - nodes_out[2 + i, pl.ds(low, 32), columns(tile)] for i in range(2)]
                top = times(rate_real, rate_imag, *own)
                offset[tile - FIRST_COARSE_TILE, 0, pl.ds(low, 32), :] = top[0] + factor * sum_imag + lead * field(tile, 0, low, low + 32)
                offset[tile - FIRST_COARSE_TILE, 1, pl.ds(low, 32), :] = top[1] - factor * sum_real + lead * field(tile, 1, low, low + 32)
            return carry

        def gather(source, target):
            return pltpu.make_async_remote_copy(
                src_ref=offset.at[piece(target)], dst_ref=gathered.at[source], send_sem=gather_send,
                recv_sem=gather_recv, device_id=in_group(target), device_id_type=MESH)

        def scatter(source, target):
            return pltpu.make_async_remote_copy(
                src_ref=results.at[target], dst_ref=begins.at[piece(source)], send_sem=scatter_send,
                recv_sem=scatter_recv, device_id=in_group(target), device_id_type=MESH)

        def hand_on(source, target):
            return pltpu.make_async_remote_copy(
                src_ref=carry_out, dst_ref=carry_in.at[source], send_sem=carry_send,
                recv_sem=carry_recv, device_id=facing(target), device_id_type=MESH)

        row = member // RING
        beside_row = (row + 1 - 2 * lax.rem(row, 2)) * RING

        def detour(stage):
            source = offset.at[piece(row * RING)] if stage == 0 else results.at[row * RING]
            sem = gather_send if stage == 0 else scatter_send
            return pltpu.make_async_remote_copy(
                src_ref=source, dst_ref=aside.at[stage], send_sem=sem, recv_sem=aside_recv.at[stage],
                device_id=in_group(beside_row), device_id_type=MESH)

        def relay_aside(stage):
            origin = beside_row + RING - 1
            target = gathered.at[origin] if stage == 0 else begins.at[piece(origin)]
            sem = gather_recv if stage == 0 else scatter_recv
            return pltpu.make_async_remote_copy(
                src_ref=aside.at[stage], dst_ref=target, send_sem=aside_send.at[stage], recv_sem=sem,
                device_id=in_group(beside_row), device_id_type=MESH)

        def crowded(stage):
            return group >= 0 if stage == 0 else group < ASIDE_GROUPS

        def pass_aside(stage):
            @pl.when((place == 0) & crowded(stage))
            def _():
                detour(stage).wait_recv()
                relay_aside(stage).start()

        def blocked(target, stage):
            return (place == RING - 1) & (target == row * RING) & crowded(stage)

        others = gathered.at[pl.ds(0, GROUP - 1)]

        def other(distance):
            return lax.rem(member + distance, GROUP)

        with jax.named_scope("full"):
            lax.fori_loop(FIRST_COARSE_TILE, FIRST_COARSE_TILE + COARSE_TILES, full, 0)
        with jax.named_scope("ready"):
            @pl.when(member < GROUP - 1)
            def _():
                pl.semaphore_wait(ready, GROUP - 1 - member)

        def spread(distance, carry):
            @pl.when(jnp.logical_not(blocked(other(distance), 0)))
            def _():
                gather(member, other(distance)).start()

            return carry

        with jax.named_scope("spread"):
            @pl.when(place == RING - 1)
            def _():
                detour(0).start()

            lax.fori_loop(1, GROUP, spread, 0)
        gathered[member] = offset[piece(member)]
        early = jnp.where(place == RING - 1, EARLY_WRAP + group * WRAP_STEP // 2, EARLY + count(place == 0) * EARLY_ZERO + group * EARLY_STEP // 2)
        early = jnp.minimum(early, TILES)
        early = jnp.maximum(early, first_pushes)
        lax.fori_loop(first_pushes, early, push_only, 0)
        with jax.named_scope("halo2"):
            wait_halo(1, 2)
        with jax.named_scope("rim"):
            lax.fori_loop(COARSE_TILES, TILES, edge, 0)
        left = pl.ds(0, FIRST_COARSE_TILE * LANES)
        right_start = (FIRST_COARSE_TILE + COARSE_TILES) * LANES
        right = pl.ds(right_start, KY - right_start)
        rims = [(upper, left), (upper, right), (lower, left), (lower, right)]
        for rows, cols in rims:
            push(rows, cols, 1)
        tile, _, _, _ = piece(member)
        first = lax.rem(member, GROUP // COARSE_TILES) * PIECE_ROWS
        rate_real, rate_imag, _ = rate_of(rank * ROWS + first, (FIRST_COARSE_TILE + tile) * LANES, PIECE_ROWS)
        gain = inverse(1.0 - rate_real, -rate_imag)

        with jax.named_scope("aside0"):
            pass_aside(0)
        with jax.named_scope("gather"):
            all_of(others, gather_send, gather_recv).wait_recv()

        def scan(index, running):
            for i in range(2):
                prefix[index, i] = running[i]
            return times(*gain, running[0] + gathered[index, 0], running[1] + gathered[index, 1])

        nothing = jnp.zeros((PIECE_ROWS, LANES), F32)
        with jax.named_scope("scan"):
            running = lax.fori_loop(0, GROUP, scan, (nothing, nothing))
            for i in range(2):
                carry_out[i] = running[i]

            @pl.when(group < groups - 1)
            def _():
                pl.semaphore_wait(ready_carry, groups - 1 - group)

            def tell(target, carry):
                hand_on(group, target).start()
                return carry

            lax.fori_loop(group + 1, groups, tell, 0)

        jump = gain
        for _ in range(GROUP.bit_length() - 1):
            jump = times(*jump, *jump)

        def join(source, running):
            far = times(*jump, *running)
            return far[0] + carry_in[source, 0], far[1] + carry_in[source, 1]

        with jax.named_scope("carry"):
            for number in range(1, groups):
                @pl.when(group == number)
                def _():
                    all_of(carry_in.at[pl.ds(0, number)], carry_send, carry_recv).wait_recv()

            entering = lax.fori_loop(0, group, join, (nothing, nothing))

        def add_carry(index, running):
            for i in range(2):
                results[index, i] = prefix[index, i] + running[i]
            return times(*gain, *running)

        lax.fori_loop(0, GROUP, add_carry, entering)

        def give(distance, carry):
            @pl.when(jnp.logical_not(blocked(other(distance), 1)))
            def _():
                scatter(member, other(distance)).start()

            return carry

        with jax.named_scope("give"):
            @pl.when((place == RING - 1) & crowded(1))
            def _():
                detour(1).start()

            lax.fori_loop(1, GROUP, give, 0)
        begins[piece(member)] = results[member]
        lax.fori_loop(early, TILES, push_only, 0)

        with jax.named_scope("aside1"):
            pass_aside(1)
        with jax.named_scope("back"):
            all_of(others, scatter_send, scatter_recv).wait_recv()

        later = 1.0 - lead

        def finish(tile, carry):
            which = tile - FIRST_COARSE_TILE
            for low in range(0, ROWS, 32):
                rows = pl.ds(low, 32)
                rate_real, rate_imag, _ = rates(tile, low, low + 32)
                inv_real, inv_imag = inverse(1.0 - rate_real, -rate_imag)
                begin_new = [begins[which, i, rows, :] for i in range(2)]
                end_new = times(inv_real, inv_imag, *[begin_new[i] + offset[which, i, rows, :] for i in range(2)])
                for i in range(2):
                    old_end = nodes_out[2 + i, rows, columns(tile)]
                    nodes_out[i, rows, columns(tile)] += 0.5 * (
                        (begin_new[i] - later * field(tile, i, low, low + 32)) + (end_new[i] - old_end))
                    nodes_out[2 + i, rows, columns(tile)] = end_new[i]
                    next_out[i, rows, columns(tile)] = begin_new[i]
            return carry

        with jax.named_scope("finish"):
            lax.fori_loop(FIRST_COARSE_TILE, FIRST_COARSE_TILE + COARSE_TILES, finish, 0)

        halo_sent()

        for number in range(1, groups):
            @pl.when(group == groups - 1 - number)
            def _():
                all_of(carry_in.at[pl.ds(0, number)], carry_send, carry_recv).wait_send()

        all_of(others, gather_send, gather_recv).wait_send()
        all_of(others, scatter_send, scatter_recv).wait_send()

        for stage in range(2):
            @pl.when((place == 0) & crowded(stage))
            def _():
                relay_aside(stage).wait_send()

        @pl.when(slot < tm_size - 1)
        def _():
            bulk(middle, pl.ds(0, FINE_TILES * LANES)).wait_send()
            bulk(pl.ds(0, 16), pl.ds(0, FINE_TILES * LANES), 1).wait_send()

        with jax.named_scope("settle"):
            settle(pl.ds(0, FINE_TILES * LANES))

    @pl.when(slot == 0)
    def _():
        def restore(tile, carry):
            for i in range(2):
                next_out[i, :, columns(tile)] = fields[tile, i, pl.ds(8, ROWS), :]
            return carry

        lax.fori_loop(0, TILES, restore, 0)


def deliver(start_ref, nodes_ref, start_hbm, nodes_hbm, sems):
    copies = [pltpu.make_async_copy(nodes_ref.at[i], nodes_hbm.at[i], sems.at[i]) for i in range(4)]
    copies += [pltpu.make_async_copy(start_ref.at[i], start_hbm.at[i], sems.at[4 + i]) for i in range(2)]
    for copy in copies:
        copy.start()
    for copy in copies:
        copy.wait()


def solution(mesh):
    tm_size, space_size = mesh.shape["tm"], mesh.shape["space"]

    def body(start_values, node_values):
        hbm = pl.BlockSpec(memory_space=pltpu.MemorySpace.HBM)
        vmem = pl.BlockSpec(memory_space=pltpu.MemorySpace.VMEM)
        dma = pltpu.SemaphoreType.DMA
        next_start, nodes = pl.pallas_call(
            functools.partial(kernel, tm_size, space_size),
            out_shape=(pltpu.MemorySpace.VMEM((2, ROWS, KY), F32), pltpu.MemorySpace.VMEM((4, ROWS, KY), F32)),
            in_specs=[hbm, hbm],
            out_specs=(vmem, vmem),
            scratch_shapes=[
                pltpu.VMEM((TILES, 6, ROWS + 16, LANES), F32),
                pltpu.VMEM((TILES, 2, ROWS + 32, LANES), F32),
                pltpu.VMEM((TILES, 2, ROWS + 32, LANES), F32),
                pltpu.VMEM((2, ROWS + 32, LANES), F32),
                pltpu.VMEM((2, ROWS + 32, LANES), F32),
                pltpu.VMEM((COARSE_TILES, 2, ROWS, LANES), F32),
                pltpu.VMEM((GROUP, 2, PIECE_ROWS, LANES), F32),
                pltpu.VMEM((GROUP, 2, PIECE_ROWS, LANES), F32),
                pltpu.VMEM((tm_size // GROUP, 2, PIECE_ROWS, LANES), F32),
                pltpu.VMEM((2, PIECE_ROWS, LANES), F32),
                pltpu.VMEM((GROUP, 2, PIECE_ROWS, LANES), F32),
                pltpu.VMEM((COARSE_TILES, 2, ROWS, LANES), F32),
                pltpu.VMEM((RELAYS, 2, RELAY_ROWS, LANES), F32),
                pltpu.VMEM((RELAYS, 2, RELAY_ROWS, LANES), F32),
                dma((TILES,)),
                dma((2,)),
                dma((2, 3)),
                dma((2,)),
                dma,
                dma,
                dma,
                dma,
                dma,
                dma,
                dma,
                dma((3,)),
                dma((2, RELAYS)),
                pltpu.SemaphoreType.REGULAR,
                pltpu.SemaphoreType.REGULAR,
                pltpu.VMEM((2, 2, PIECE_ROWS, LANES), F32),
                dma((2,)),
                dma((2,)),
            ],
            compiler_params=pltpu.CompilerParams(collective_id=0, has_side_effects=True, vmem_limit_bytes=61696 * 1024),
            name="pfasst",
        )(start_values[0], node_values[0].reshape(4, ROWS, KY))
        next_start, nodes = pl.pallas_call(
            deliver,
            out_shape=(jax.ShapeDtypeStruct((2, ROWS, KY), F32), jax.ShapeDtypeStruct((4, ROWS, KY), F32)),
            in_specs=[vmem, vmem],
            out_specs=(hbm, hbm),
            scratch_shapes=[dma((6,))],
            compiler_params=pltpu.CompilerParams(vmem_limit_bytes=2**20),
            name="deliver",
        )(next_start, nodes)
        return next_start[None], nodes.reshape(1, 2, 2, ROWS, KY)

    return jax.shard_map(
        body,
        mesh=mesh,
        in_specs=(P("tm", None, "space", None), P("tm", None, None, "space", None)),
        out_specs=(P("tm", None, "space", None), P("tm", None, None, "space", None)),
        check_vma=False,
    )
```

```python
import functools

import jax
import jax.numpy as jnp
from jax import lax
from jax.experimental import pallas as pl
from jax.experimental.pallas import tpu as pltpu
from jax.sharding import PartitionSpec as P

MESH = pl.DeviceIdType.MESH
F32 = jnp.float32
KX = 1024
KY = 1024
CX = 256
LANES = 128
ROWS = 128
TILES = KY // LANES
FIRST_COARSE_TILE = (KY // 2 - CX // 2) // LANES
COARSE_TILES = CX // LANES
FIRST_COARSE_RANK = (KX // 2 - CX // 2) // ROWS
COARSE_RANKS = CX // ROWS
FINE_TILES = TILES - COARSE_TILES
RING = 4
GROUP = 8
PIECE_ROWS = COARSE_TILES * ROWS // GROUP
RELAY_SHARED = 2
RELAY_WRAP = 1
RELAY_BOTH = 3
RELAYS = 4 + RELAY_SHARED + RELAY_WRAP + RELAY_BOTH
RELAY_ROWS = 56
EARLY = 4
EARLY_WRAP = 5
EARLY_STEP = 1
WRAP_STEP = 1
LAST_WRAP = 2
LAST_FIRST = 0
LEAD = 1
DELIVER_ROWS = 32
EARLY_ZERO = 2
LAG = 6
FIRST = 2
FIRST_WRAP = 2

diffusion = 1.5
drift = 0.8
shear = 0.6


def columns(tile):
    return pl.ds(pl.multiple_of(tile * LANES, LANES), LANES)


def rate_of(first_row, first_column, rows):
    row = (first_row + lax.broadcasted_iota(jnp.int32, (rows, LANES), 0)).astype(F32)
    column = (first_column + lax.broadcasted_iota(jnp.int32, (rows, LANES), 1)).astype(F32)
    along = (row - KX // 2) / (KX // 2)
    across = (column - KY // 2) / (KY // 2)
    return -diffusion * (along * along + across * across), -drift * across, shear * across


def times(ar, ai, br, bi):
    return ar * br - ai * bi, ar * bi + ai * br


def inverse(real_part, imag_part):
    scale = 1.0 / (real_part * real_part + imag_part * imag_part)
    return real_part * scale, -imag_part * scale


def tile_at(index):
    early = jnp.where(index < COARSE_TILES, index + FIRST_COARSE_TILE, index - COARSE_TILES)
    return jnp.where(index < FIRST_COARSE_TILE + COARSE_TILES, early, index)


def kernel(tm_size, space_size, start_hbm, nodes_hbm, next_out, nodes_out, fields, mixed, staged, node_one_buf, whole, offset,
           gathered, prefix, carry_in, carry_out, results, begins, first_leg, second_leg, load_sem, halo_send, halo_recv, bulk_send,
           bulk_recv, gather_send, gather_recv, carry_send, carry_recv, scatter_send, scatter_recv, relay_send, relay_recv,
           ready, ready_carry, aside, aside_send, aside_recv):
    slot = lax.axis_index("tm")
    rank = lax.axis_index("space")
    coarse = (rank >= FIRST_COARSE_RANK) & (rank < FIRST_COARSE_RANK + COARSE_RANKS)
    fine = jnp.logical_not(coarse)
    shared = (rank == FIRST_COARSE_RANK - 1) | (rank == FIRST_COARSE_RANK + COARSE_RANKS)
    column, place = slot // RING, lax.rem(slot, RING)

    def at_slot(index):
        return {"tm": lax.rem(index, tm_size), "space": rank}

    after = slot + 1
    before = slot + tm_size - 1
    above = column * RING + lax.rem(place + 1, RING)
    below = column * RING + lax.rem(place + RING - 1, RING)

    def loads(tile):
        body = pl.ds(8, ROWS)
        return (
            pltpu.make_async_copy(start_hbm.at[:, :, columns(tile)], fields.at[tile, pl.ds(0, 2), body, :], load_sem.at[tile]),
            pltpu.make_async_copy(nodes_hbm.at[:, :, columns(tile)], fields.at[tile, pl.ds(2, 4), body, :], load_sem.at[tile]),
        )

    def wait_load(tile):
        landed = fields.at[tile, :, pl.ds(8, ROWS), :]
        pltpu.make_async_copy(landed, landed, load_sem.at[tile]).wait()

    barrier = pltpu.get_barrier_semaphore()

    def greet(target):
        pl.semaphore_signal(barrier, inc=1, device_id=target, device_id_type=MESH)

    @pl.when(rank > 0)
    def _():
        greet({"tm": slot, "space": rank - 1})

    @pl.when(rank < space_size - 1)
    def _():
        greet({"tm": slot, "space": rank + 1})

    greet(at_slot(before))

    @pl.when(fine)
    def _():
        greet(at_slot(above))

        @pl.when(place == 0)
        def _():
            greet(at_slot(slot + tm_size - RING + 1))

    member, group = lax.rem(slot, GROUP), slot // GROUP
    groups = tm_size // GROUP
    def in_group(index):
        return at_slot(group * GROUP + index)

    def facing(index):
        return at_slot(index * GROUP + member)

    @pl.when(coarse)
    def _():
        def call(index, carry):
            greet(in_group(index))
            return carry

        lax.fori_loop(member + 1, GROUP, call, 0)

        def call_later(index, carry):
            greet(facing(index))
            return carry

        lax.fori_loop(group + 1, groups, call_later, 0)

    def begin_load(index, carry):
        for copy in loads(tile_at(index)):
            copy.start()
        return carry

    lax.fori_loop(0, TILES, begin_load, 0)
    mixed[:, :, pl.ds(8, 8), :] = jnp.zeros((TILES, 2, 8, LANES), F32)
    mixed[:, :, pl.ds(144, 8), :] = jnp.zeros((TILES, 2, 8, LANES), F32)

    with jax.named_scope("load"):
        for tile in range(FIRST_COARSE_TILE, FIRST_COARSE_TILE + COARSE_TILES):
            wait_load(tile)

    def count(flag):
        return flag.astype(jnp.int32)

    with jax.named_scope("barrier"):
        own_kind = jnp.where(coarse, member + group, 1 + count(place == 1))
        pl.semaphore_wait(barrier, 1 + count(rank > 0) + count(rank < space_size - 1) + own_kind)

    @pl.when(coarse)
    def _():
        def answer_earlier(index, carry):
            pl.semaphore_signal(ready_carry, inc=1, device_id=facing(index), device_id_type=MESH)
            return carry

        lax.fori_loop(0, group, answer_earlier, 0)

        def answer(index, carry):
            pl.semaphore_signal(ready, inc=1, device_id=in_group(index), device_id_type=MESH)
            return carry

        lax.fori_loop(0, member, answer, 0)

    parts = (pl.ds(FIRST_COARSE_TILE, COARSE_TILES), pl.ds(0, FIRST_COARSE_TILE),
             pl.ds(FIRST_COARSE_TILE + COARSE_TILES, TILES - FIRST_COARSE_TILE - COARSE_TILES))

    def halo(side, part):
        low, high = (ROWS, 0) if side == 0 else (8, ROWS + 8)
        return pltpu.make_async_remote_copy(
            src_ref=fields.at[parts[part], :, pl.ds(low, 8), :], dst_ref=fields.at[parts[part], :, pl.ds(high, 8), :],
            send_sem=halo_send.at[side], recv_sem=halo_recv.at[side, part],
            device_id={"tm": slot, "space": rank + 1 if side == 0 else rank - 1}, device_id_type=MESH)

    def send_halo(*which):
        @pl.when(rank < space_size - 1)
        def _():
            for part in which:
                halo(0, part).start()

        @pl.when(rank > 0)
        def _():
            for part in which:
                halo(1, part).start()

    def wait_halo(*which):
        @pl.when(rank > 0)
        def _():
            for part in which:
                halo(0, part).wait_recv()

        @pl.when(rank < space_size - 1)
        def _():
            for part in which:
                halo(1, part).wait_recv()

    def all_of(ref, send, recv):
        return pltpu.make_async_remote_copy(
            src_ref=ref, dst_ref=ref, send_sem=send, recv_sem=recv, device_id=at_slot(after), device_id_type=MESH)

    def halo_sent():
        edge_rows = fields.at[:, :, pl.ds(0, 8), :]

        @pl.when(rank < space_size - 1)
        def _():
            all_of(edge_rows, halo_send.at[0], halo_recv.at[0, 0]).wait_send()

        @pl.when(rank > 0)
        def _():
            all_of(edge_rows, halo_send.at[1], halo_recv.at[0, 0]).wait_send()

    send_halo(0)

    def bulk(rows, cols, index=0):
        return pltpu.make_async_remote_copy(
            src_ref=nodes_out.at[pl.ds(2, 2), rows, cols], dst_ref=next_out.at[:, rows, cols],
            send_sem=bulk_send.at[index], recv_sem=bulk_recv, device_id=at_slot(after), device_id_type=MESH)

    def push(rows, cols, index=0):
        @pl.when(slot < tm_size - 1)
        def _():
            bulk(rows, cols, index).start()

    def field(tile, plane, low, high):
        return fields[tile, plane, pl.ds(low + 8, high - low), :]

    def mix(tile, low, high):
        for part in range(2):
            mixed[tile, part, pl.ds(low + 16, high - low), :] = (
                (5.0 / 24.0) * field(tile, part, low, high) + (1.0 / 3.0) * field(tile, 2 + part, low, high)
                - (1.0 / 24.0) * field(tile, 4 + part, low, high))

    def beside(ref, lead, low, high):
        count = high - low
        real = ref[(*lead, 0, pl.ds(low + 15, count), slice(None))] + ref[(*lead, 0, pl.ds(low + 17, count), slice(None))]
        imag = ref[(*lead, 1, pl.ds(low + 15, count), slice(None))] + ref[(*lead, 1, pl.ds(low + 17, count), slice(None))]
        return real, imag

    def rates(tile, low, high):
        return rate_of(rank * ROWS + low, tile * LANES, high - low)

    def one(tile, low, high, scale=None, keep=False):
        rate_real, rate_imag, factor = rates(tile, low, high)
        inv_real, inv_imag = inverse(1.0 - 0.5 * rate_real, -0.5 * rate_imag)
        sum_real, sum_imag = beside(mixed, (tile,), low, high)
        begin = [field(tile, part, low, high) for part in range(2)]
        old_one = [field(tile, 2 + part, low, high) for part in range(2)]
        old_two = [field(tile, 4 + part, low, high) for part in range(2)]
        own = [(5.0 / 24.0) * begin[i] - (1.0 / 6.0) * old_one[i] - (1.0 / 24.0) * old_two[i] for i in range(2)]
        top = times(rate_real, rate_imag, *own)
        node = times(inv_real, inv_imag, begin[0] + top[0] + factor * sum_imag, begin[1] + top[1] - factor * sum_real)
        if scale is not None:
            node = [part * scale for part in node]
        for i in range(2):
            staged[tile, i, pl.ds(low + 16, high - low), :] = (
                (5.0 / 24.0) * old_two[i] - (1.0 / 24.0) * begin[i] - (1.0 / 6.0) * old_one[i] + 0.5 * node[i])
            if keep:
                node_one_buf[i, pl.ds(low + 16, high - low), :] = node[i]
            first, last = max(low, 0), min(high, ROWS)
            if first < last:
                nodes_out[i, pl.ds(first, last - first), columns(tile)] = node[i][first - low:last - low]

    def two(tile, low, high, keep=False):
        rate_real, rate_imag, factor = rates(tile, low, high)
        inv_real, inv_imag = inverse(1.0 - 0.5 * rate_real, -0.5 * rate_imag)
        sum_real, sum_imag = beside(staged, (tile,), low, high)
        begin = [field(tile, part, low, high) for part in range(2)]
        old_one = [field(tile, 2 + part, low, high) for part in range(2)]
        old_two = [field(tile, 4 + part, low, high) for part in range(2)]
        if keep:
            node = [node_one_buf[i, pl.ds(low + 16, high - low), :] for i in range(2)]
        else:
            node = [nodes_out[i, pl.ds(low, high - low), columns(tile)] for i in range(2)]
        own = [(1.0 / 3.0) * old_one[i] - (1.0 / 24.0) * begin[i] - (7.0 / 24.0) * old_two[i] for i in range(2)]
        top = times(rate_real, rate_imag, *own)
        last_node = times(inv_real, inv_imag, node[0] + top[0] + factor * sum_imag, node[1] + top[1] - factor * sum_real)
        for i in range(2):
            if keep:
                whole[i, pl.ds(low + 16, high - low), :] = (
                    (1.0 / 6.0) * begin[i] + (2.0 / 3.0) * node[i] + (1.0 / 6.0) * last_node[i])
            first, last = max(low, 0), min(high, ROWS)
            if first < last:
                nodes_out[2 + i, pl.ds(first, last - first), columns(tile)] = last_node[i][first - low:last - low]

    def inner(tile):
        for low in range(0, ROWS, 32):
            mix(tile, low, low + 32)
        for low in range(0, ROWS, 32):
            one(tile, low, low + 32)
        for low in (8, 40, 72, 104):
            two(tile, low, min(low + 32, 120))

    def rim(tile):
        mix(tile, -8, 0)
        mix(tile, ROWS, ROWS + 8)
        one(tile, -8, 8, scale=jnp.concatenate([jnp.full((8, LANES), (rank > 0).astype(F32)), jnp.ones((8, LANES), F32)]))
        one(tile, 120, 136,
            scale=jnp.concatenate([jnp.ones((8, LANES), F32), jnp.full((8, LANES), (rank < space_size - 1).astype(F32))]))
        two(tile, 0, 8)
        two(tile, 120, 128)

    middle = pl.ds(8, 112)
    upper = pl.ds(0, 8)
    lower = pl.ds(120, 8)

    def edge(index, carry):
        rim(tile_at(index))
        return carry

    def settle(cols):
        @pl.when(slot > 0)
        def _():
            bulk(slice(None), cols).wait_recv()

    @pl.when(fine)
    def _():
        def relay_source(chunk):
            rows = pl.ds(pl.multiple_of(8 + lax.rem(chunk, 2) * RELAY_ROWS, 8), RELAY_ROWS)
            return rows, columns(tile_at(LEAD + chunk // 2))

        def leg(which, chunk):
            rows, cols = relay_source(chunk)
            if which == 0:
                source, target, device = nodes_out.at[pl.ds(2, 2), rows, cols], first_leg.at[chunk], at_slot(below)
                recv = relay_recv.at[0, chunk]
            elif which == 1:
                source, target, device, recv = first_leg.at[chunk], second_leg.at[chunk], at_slot(below), relay_recv.at[1, chunk]
            else:
                origin = column * RING + lax.rem(place + 2, RING)
                source, target, device, recv = second_leg.at[chunk], next_out.at[:, rows, cols], at_slot(origin + 1), bulk_recv
            return pltpu.make_async_remote_copy(
                src_ref=source, dst_ref=target, send_sem=relay_send.at[which], recv_sem=recv,
                device_id=device, device_id_type=MESH)

        def relayed(which):
            start = lax.rem(place + which, RING)
            wraps = (start == RING - 1).astype(jnp.int32)
            return 4 + RELAY_WRAP * wraps + count(shared) * (RELAY_SHARED + RELAY_BOTH * wraps)

        def has_origin(which):
            return column * RING + lax.rem(place + which, RING) < tm_size - 1

        def start_tile(index, carry):
            @pl.when(index >= COARSE_TILES)
            def _():
                wait_load(tile_at(index))

            inner(tile_at(index))
            first = 2 * (index - LEAD)
            chunks = jnp.where(first < 0, 0, relayed(0) - first)

            @pl.when(has_origin(0) & (chunks > 0))
            def _():
                leg(0, first).start()

            @pl.when(has_origin(0) & (chunks > 1))
            def _():
                leg(0, first + 1).start()

            @pl.when(has_origin(0) & (chunks == 1))
            def _():
                bulk(pl.ds(8 + RELAY_ROWS, RELAY_ROWS), columns(tile_at(index))).start()

            @pl.when(has_origin(0) & (chunks <= 0))
            def _():
                bulk(middle, columns(tile_at(index))).start()

            return carry

        def forward(which, chunk):
            @pl.when(has_origin(which) & (chunk >= 0) & (chunk < relayed(which)))
            def _():
                leg(which - 1, chunk).wait_recv()
                leg(which, chunk).start()

        with jax.named_scope("inner"):
            lax.fori_loop(0, TILES, start_tile, 0)
        send_halo(1, 2)
        with jax.named_scope("fwdA"):
            forward(1, 0)
            forward(1, 1)
        with jax.named_scope("halo"):
            wait_halo(0, 1, 2)

        @pl.when(rank == 0)
        def _():
            fields[:, :, pl.ds(0, 8), :] = jnp.zeros((TILES, 6, 8, LANES), F32)

        @pl.when(rank == space_size - 1)
        def _():
            fields[:, :, pl.ds(ROWS + 8, 8), :] = jnp.zeros((TILES, 6, 8, LANES), F32)

        with jax.named_scope("rim"):
            lax.fori_loop(0, TILES, edge, 0)
        push(upper, slice(None), 1)
        push(lower, slice(None), 1)

        def pass_on(step, carry):
            forward(1, step)
            forward(2, step - LAG)
            return carry

        with jax.named_scope("fwdB"):
            lax.fori_loop(2, RELAYS + LAG, pass_on, 0)
        halo_sent()

        for relays in range(4, RELAYS + 1):
            chunks = first_leg.at[pl.ds(0, relays)]
            direct = fields.at[pl.ds(0, 7), pl.ds(0, 2), pl.ds(0, 8 * (2 * TILES - relays)), :]
            for which in range(3):
                @pl.when(has_origin(which) & (relayed(which) == relays))
                def _():
                    all_of(chunks, relay_send.at[which], relay_recv.at[0, 0]).wait_send()

            @pl.when(has_origin(0) & (relayed(0) == relays))
            def _():
                all_of(direct, bulk_send.at[0], relay_recv.at[0, 0]).wait_send()

        @pl.when(has_origin(0))
        def _():
            bulk(pl.ds(0, 16), slice(None), 1).wait_send()

        with jax.named_scope("settle"):
            settle(slice(None))

    @pl.when(coarse)
    def _():
        lead = (slot == 0).astype(F32)

        def piece(index):
            share = GROUP // COARSE_TILES
            rows = pl.ds(pl.multiple_of(lax.rem(index, share) * PIECE_ROWS, 8), PIECE_ROWS)
            return index // share, slice(None), rows, slice(None)

        def push_only(index, carry):
            push(middle, columns(tile_at(index)))
            return carry

        lax.fori_loop(COARSE_TILES, TILES, lambda index, carry: (wait_load(tile_at(index)), carry)[1], 0)
        send_halo(1, 2)
        with jax.named_scope("innerA"):
            def inner_and_push(index, carry):
                inner(tile_at(index))

                @pl.when(index < first_pushes)
                def _():
                    push_only(index, 0)

                return carry

            first_pushes = COARSE_TILES + jnp.where(place == RING - 1, FIRST_WRAP + LAST_FIRST * count(group == groups - 1), FIRST)
            lax.fori_loop(COARSE_TILES, TILES, inner_and_push, 0)
        with jax.named_scope("halo"):
            wait_halo(0)

        def full(tile, carry):
            bands = ((-8, 24), (24, 56), (56, 88), (88, 120), (120, 136))
            for low, high in bands:
                mix(tile, low, high)
            for low, high in bands:
                one(tile, low, high, keep=True)
            for low, high in bands:
                two(tile, low, high, keep=True)
            for low in range(0, ROWS, 32):
                rate_real, rate_imag, factor = rates(tile, low, low + 32)
                sum_real, sum_imag = beside(whole, (), low, low + 32)
                own = [whole[i, pl.ds(low + 16, 32), :] - nodes_out[2 + i, pl.ds(low, 32), columns(tile)] for i in range(2)]
                top = times(rate_real, rate_imag, *own)
                offset[tile - FIRST_COARSE_TILE, 0, pl.ds(low, 32), :] = top[0] + factor * sum_imag + lead * field(tile, 0, low, low + 32)
                offset[tile - FIRST_COARSE_TILE, 1, pl.ds(low, 32), :] = top[1] - factor * sum_real + lead * field(tile, 1, low, low + 32)
            return carry

        def gather(source, target):
            return pltpu.make_async_remote_copy(
                src_ref=offset.at[piece(target)], dst_ref=gathered.at[source], send_sem=gather_send,
                recv_sem=gather_recv, device_id=in_group(target), device_id_type=MESH)

        def scatter(source, target):
            return pltpu.make_async_remote_copy(
                src_ref=results.at[target], dst_ref=begins.at[piece(source)], send_sem=scatter_send,
                recv_sem=scatter_recv, device_id=in_group(target), device_id_type=MESH)

        def hand_on(source, target):
            return pltpu.make_async_remote_copy(
                src_ref=carry_out, dst_ref=carry_in.at[source], send_sem=carry_send,
                recv_sem=carry_recv, device_id=facing(target), device_id_type=MESH)

        row = member // RING
        beside_row = (row + 1 - 2 * lax.rem(row, 2)) * RING

        def detour(stage):
            source = offset.at[piece(row * RING)] if stage == 0 else results.at[row * RING]
            sem = gather_send if stage == 0 else scatter_send
            return pltpu.make_async_remote_copy(
                src_ref=source, dst_ref=aside.at[stage], send_sem=sem, recv_sem=aside_recv.at[stage],
                device_id=in_group(beside_row), device_id_type=MESH)

        def relay_aside(stage):
            origin = beside_row + RING - 1
            target = gathered.at[origin] if stage == 0 else begins.at[piece(origin)]
            sem = gather_recv if stage == 0 else scatter_recv
            return pltpu.make_async_remote_copy(
                src_ref=aside.at[stage], dst_ref=target, send_sem=aside_send.at[stage], recv_sem=sem,
                device_id=in_group(beside_row), device_id_type=MESH)

        def crowded(stage, row):
            return (group > 0) & (row == 0) if stage == 0 else (group == 0) & (row == 1)

        def pass_aside(stage):
            @pl.when((place == 0) & crowded(stage, 1 - row))
            def _():
                detour(stage).wait_recv()
                relay_aside(stage).start()

        def blocked(target, stage):
            return (place == RING - 1) & (target == row * RING) & crowded(stage, row)

        others = gathered.at[pl.ds(0, GROUP - 1)]

        def other(distance):
            return lax.rem(member + distance, GROUP)

        with jax.named_scope("full"):
            lax.fori_loop(FIRST_COARSE_TILE, FIRST_COARSE_TILE + COARSE_TILES, full, 0)
        with jax.named_scope("ready"):
            @pl.when(member < GROUP - 1)
            def _():
                pl.semaphore_wait(ready, GROUP - 1 - member)

        def spread(distance, carry):
            @pl.when(jnp.logical_not(blocked(other(distance), 0)))
            def _():
                gather(member, other(distance)).start()

            return carry

        with jax.named_scope("spread"):
            @pl.when((place == RING - 1) & crowded(0, row))
            def _():
                detour(0).start()

            lax.fori_loop(1, GROUP, spread, 0)
        gathered[member] = offset[piece(member)]
        early = jnp.where(place == RING - 1, EARLY_WRAP + group * WRAP_STEP // 2, EARLY + count(place == 0) * EARLY_ZERO + group * EARLY_STEP // 2)
        early = jnp.minimum(early + LAST_WRAP * count((place == RING - 1) & (group == groups - 1)), TILES)
        early = jnp.maximum(early, first_pushes)
        lax.fori_loop(first_pushes, early, push_only, 0)
        with jax.named_scope("halo2"):
            wait_halo(1, 2)
        with jax.named_scope("rim"):
            lax.fori_loop(COARSE_TILES, TILES, edge, 0)
        left = pl.ds(0, FIRST_COARSE_TILE * LANES)
        right_start = (FIRST_COARSE_TILE + COARSE_TILES) * LANES
        right = pl.ds(right_start, KY - right_start)
        rims = [(upper, left), (upper, right), (lower, left), (lower, right)]
        for rows, cols in rims:
            push(rows, cols, 1)
        tile, _, _, _ = piece(member)
        first = lax.rem(member, GROUP // COARSE_TILES) * PIECE_ROWS
        rate_real, rate_imag, _ = rate_of(rank * ROWS + first, (FIRST_COARSE_TILE + tile) * LANES, PIECE_ROWS)
        gain = inverse(1.0 - rate_real, -rate_imag)

        with jax.named_scope("aside0"):
            pass_aside(0)
        with jax.named_scope("gather"):
            all_of(others, gather_send, gather_recv).wait_recv()

        def scan(index, running):
            for i in range(2):
                prefix[index, i] = running[i]
            return times(*gain, running[0] + gathered[index, 0], running[1] + gathered[index, 1])

        nothing = jnp.zeros((PIECE_ROWS, LANES), F32)
        with jax.named_scope("scan"):
            running = lax.fori_loop(0, GROUP, scan, (nothing, nothing))
            for i in range(2):
                carry_out[i] = running[i]

            @pl.when(group < groups - 1)
            def _():
                pl.semaphore_wait(ready_carry, groups - 1 - group)

            def tell(target, carry):
                hand_on(group, target).start()
                return carry

            lax.fori_loop(group + 1, groups, tell, 0)

        jump = gain
        for _ in range(GROUP.bit_length() - 1):
            jump = times(*jump, *jump)

        def join(source, running):
            far = times(*jump, *running)
            return far[0] + carry_in[source, 0], far[1] + carry_in[source, 1]

        with jax.named_scope("carry"):
            for number in range(1, groups):
                @pl.when(group == number)
                def _():
                    all_of(carry_in.at[pl.ds(0, number)], carry_send, carry_recv).wait_recv()

            entering = lax.fori_loop(0, group, join, (nothing, nothing))

        def add_carry(index, running):
            for i in range(2):
                results[index, i] = prefix[index, i] + running[i]
            return times(*gain, *running)

        lax.fori_loop(0, GROUP, add_carry, entering)

        def give(distance, carry):
            @pl.when(jnp.logical_not(blocked(other(distance), 1)))
            def _():
                scatter(member, other(distance)).start()

            return carry

        with jax.named_scope("give"):
            @pl.when((place == RING - 1) & crowded(1, row))
            def _():
                detour(1).start()

            lax.fori_loop(1, GROUP, give, 0)
        begins[piece(member)] = results[member]
        lax.fori_loop(early, TILES, push_only, 0)

        with jax.named_scope("aside1"):
            pass_aside(1)
        with jax.named_scope("back"):
            all_of(others, scatter_send, scatter_recv).wait_recv()

        later = 1.0 - lead

        def finish(tile, carry):
            which = tile - FIRST_COARSE_TILE
            for low in range(0, ROWS, 32):
                rows = pl.ds(low, 32)
                rate_real, rate_imag, _ = rates(tile, low, low + 32)
                inv_real, inv_imag = inverse(1.0 - rate_real, -rate_imag)
                begin_new = [begins[which, i, rows, :] for i in range(2)]
                end_new = times(inv_real, inv_imag, *[begin_new[i] + offset[which, i, rows, :] for i in range(2)])
                for i in range(2):
                    old_end = nodes_out[2 + i, rows, columns(tile)]
                    nodes_out[i, rows, columns(tile)] += 0.5 * (
                        (begin_new[i] - later * field(tile, i, low, low + 32)) + (end_new[i] - old_end))
                    nodes_out[2 + i, rows, columns(tile)] = end_new[i]
                    next_out[i, rows, columns(tile)] = begin_new[i]
            return carry

        with jax.named_scope("finish"):
            lax.fori_loop(FIRST_COARSE_TILE, FIRST_COARSE_TILE + COARSE_TILES, finish, 0)

        halo_sent()

        for number in range(1, groups):
            @pl.when(group == groups - 1 - number)
            def _():
                all_of(carry_in.at[pl.ds(0, number)], carry_send, carry_recv).wait_send()

        all_of(others, gather_send, gather_recv).wait_send()
        all_of(others, scatter_send, scatter_recv).wait_send()

        for stage in range(2):
            @pl.when((place == 0) & crowded(stage, 1 - row))
            def _():
                relay_aside(stage).wait_send()

        @pl.when(slot < tm_size - 1)
        def _():
            bulk(middle, pl.ds(0, FINE_TILES * LANES)).wait_send()
            bulk(pl.ds(0, 16), pl.ds(0, FINE_TILES * LANES), 1).wait_send()

        with jax.named_scope("settle"):
            settle(pl.ds(0, FINE_TILES * LANES))

    @pl.when(slot == 0)
    def _():
        def restore(tile, carry):
            for i in range(2):
                next_out[i, :, columns(tile)] = fields[tile, i, pl.ds(8, ROWS), :]
            return carry

        lax.fori_loop(0, TILES, restore, 0)


def deliver(start_ref, nodes_ref, start_hbm, nodes_hbm, sem):
    def copies(source, target, planes):
        return [pltpu.make_async_copy(source.at[i, pl.ds(row, DELIVER_ROWS)], target.at[i, pl.ds(row, DELIVER_ROWS)], sem)
                for i in range(planes) for row in range(0, ROWS, DELIVER_ROWS)]

    for copy in copies(nodes_ref, nodes_hbm, 4) + copies(start_ref, start_hbm, 2):
        copy.start()
    pltpu.make_async_copy(nodes_ref, nodes_hbm, sem).wait()
    pltpu.make_async_copy(start_ref, start_hbm, sem).wait()


def solution(mesh):
    tm_size, space_size = mesh.shape["tm"], mesh.shape["space"]

    def body(start_values, node_values):
        hbm = pl.BlockSpec(memory_space=pltpu.MemorySpace.HBM)
        vmem = pl.BlockSpec(memory_space=pltpu.MemorySpace.VMEM)
        dma = pltpu.SemaphoreType.DMA
        next_start, nodes = pl.pallas_call(
            functools.partial(kernel, tm_size, space_size),
            out_shape=(pltpu.MemorySpace.VMEM((2, ROWS, KY), F32), pltpu.MemorySpace.VMEM((4, ROWS, KY), F32)),
            in_specs=[hbm, hbm],
            out_specs=(vmem, vmem),
            scratch_shapes=[
                pltpu.VMEM((TILES, 6, ROWS + 16, LANES), F32),
                pltpu.VMEM((TILES, 2, ROWS + 32, LANES), F32),
                pltpu.VMEM((TILES, 2, ROWS + 32, LANES), F32),
                pltpu.VMEM((2, ROWS + 32, LANES), F32),
                pltpu.VMEM((2, ROWS + 32, LANES), F32),
                pltpu.VMEM((COARSE_TILES, 2, ROWS, LANES), F32),
                pltpu.VMEM((GROUP, 2, PIECE_ROWS, LANES), F32),
                pltpu.VMEM((GROUP, 2, PIECE_ROWS, LANES), F32),
                pltpu.VMEM((tm_size // GROUP, 2, PIECE_ROWS, LANES), F32),
                pltpu.VMEM((2, PIECE_ROWS, LANES), F32),
                pltpu.VMEM((GROUP, 2, PIECE_ROWS, LANES), F32),
                pltpu.VMEM((COARSE_TILES, 2, ROWS, LANES), F32),
                pltpu.VMEM((RELAYS, 2, RELAY_ROWS, LANES), F32),
                pltpu.VMEM((RELAYS, 2, RELAY_ROWS, LANES), F32),
                dma((TILES,)),
                dma((2,)),
                dma((2, 3)),
                dma((2,)),
                dma,
                dma,
                dma,
                dma,
                dma,
                dma,
                dma,
                dma((3,)),
                dma((2, RELAYS)),
                pltpu.SemaphoreType.REGULAR,
                pltpu.SemaphoreType.REGULAR,
                pltpu.VMEM((2, 2, PIECE_ROWS, LANES), F32),
                dma((2,)),
                dma((2,)),
            ],
            compiler_params=pltpu.CompilerParams(collective_id=0, has_side_effects=True, vmem_limit_bytes=61696 * 1024),
            name="pfasst",
        )(start_values[0], node_values[0].reshape(4, ROWS, KY))
        next_start, nodes = pl.pallas_call(
            deliver,
            out_shape=(jax.ShapeDtypeStruct((2, ROWS, KY), F32), jax.ShapeDtypeStruct((4, ROWS, KY), F32)),
            in_specs=[vmem, vmem],
            out_specs=(hbm, hbm),
            scratch_shapes=[dma],
            compiler_params=pltpu.CompilerParams(vmem_limit_bytes=2**20),
            name="deliver",
        )(next_start, nodes)
        return next_start[None], nodes.reshape(1, 2, 2, ROWS, KY)

    return jax.shard_map(
        body,
        mesh=mesh,
        in_specs=(P("tm", None, "space", None), P("tm", None, None, "space", None)),
        out_specs=(P("tm", None, "space", None), P("tm", None, None, "space", None)),
        check_vma=False,
    )
```

```python
import functools

import jax
import jax.numpy as jnp
from jax import lax
from jax.experimental import pallas as pl
from jax.experimental.pallas import tpu as pltpu
from jax.sharding import PartitionSpec as P

MESH = pl.DeviceIdType.MESH
F32 = jnp.float32
KX = 1024
KY = 1024
CX = 256
LANES = 128
ROWS = 128
TILES = KY // LANES
FIRST_COARSE_TILE = (KY // 2 - CX // 2) // LANES
COARSE_TILES = CX // LANES
FIRST_COARSE_RANK = (KX // 2 - CX // 2) // ROWS
COARSE_RANKS = CX // ROWS
FINE_TILES = TILES - COARSE_TILES
RING = 4
GROUP = 8
PIECE_ROWS = COARSE_TILES * ROWS // GROUP
RELAY_SHARED = 2
RELAY_WRAP = 1
RELAY_BOTH = 3
RELAYS = 4 + RELAY_SHARED + RELAY_WRAP + RELAY_BOTH
RELAY_ROWS = 56
EARLY = 4
EARLY_WRAP = 5
EARLY_STEP = 1
WRAP_STEP = 1
LAST_WRAP = 2
LAST_FIRST = 0
LEAD = 1
DELIVER_ROWS = 16
EARLY_ZERO = 2
LAG = 6
FIRST = 2
FIRST_WRAP = 2

diffusion = 1.5
drift = 0.8
shear = 0.6


def columns(tile):
    return pl.ds(pl.multiple_of(tile * LANES, LANES), LANES)


def rate_of(first_row, first_column, rows):
    row = (first_row + lax.broadcasted_iota(jnp.int32, (rows, LANES), 0)).astype(F32)
    column = (first_column + lax.broadcasted_iota(jnp.int32, (rows, LANES), 1)).astype(F32)
    along = (row - KX // 2) / (KX // 2)
    across = (column - KY // 2) / (KY // 2)
    return -diffusion * (along * along + across * across), -drift * across, shear * across


def times(ar, ai, br, bi):
    return ar * br - ai * bi, ar * bi + ai * br


def inverse(real_part, imag_part):
    scale = 1.0 / (real_part * real_part + imag_part * imag_part)
    return real_part * scale, -imag_part * scale


def tile_at(index):
    early = jnp.where(index < COARSE_TILES, index + FIRST_COARSE_TILE, index - COARSE_TILES)
    return jnp.where(index < FIRST_COARSE_TILE + COARSE_TILES, early, index)


def kernel(tm_size, space_size, start_hbm, nodes_hbm, next_out, nodes_out, fields, mixed, staged, node_one_buf, whole, offset,
           gathered, prefix, carry_in, carry_out, results, begins, first_leg, second_leg, load_sem, halo_send, halo_recv, bulk_send,
           bulk_recv, gather_send, gather_recv, carry_send, carry_recv, scatter_send, scatter_recv, relay_send, relay_recv,
           ready, ready_carry, aside, aside_send, aside_recv):
    slot = lax.axis_index("tm")
    rank = lax.axis_index("space")
    coarse = (rank >= FIRST_COARSE_RANK) & (rank < FIRST_COARSE_RANK + COARSE_RANKS)
    fine = jnp.logical_not(coarse)
    shared = (rank == FIRST_COARSE_RANK - 1) | (rank == FIRST_COARSE_RANK + COARSE_RANKS)
    column, place = slot // RING, lax.rem(slot, RING)

    def at_slot(index):
        return {"tm": lax.rem(index, tm_size), "space": rank}

    after = slot + 1
    before = slot + tm_size - 1
    above = column * RING + lax.rem(place + 1, RING)
    below = column * RING + lax.rem(place + RING - 1, RING)

    def loads(tile):
        body = pl.ds(8, ROWS)
        return (
            pltpu.make_async_copy(start_hbm.at[:, :, columns(tile)], fields.at[tile, pl.ds(0, 2), body, :], load_sem.at[tile]),
            pltpu.make_async_copy(nodes_hbm.at[:, :, columns(tile)], fields.at[tile, pl.ds(2, 4), body, :], load_sem.at[tile]),
        )

    def wait_load(tile):
        landed = fields.at[tile, :, pl.ds(8, ROWS), :]
        pltpu.make_async_copy(landed, landed, load_sem.at[tile]).wait()

    barrier = pltpu.get_barrier_semaphore()

    def greet(target):
        pl.semaphore_signal(barrier, inc=1, device_id=target, device_id_type=MESH)

    @pl.when(rank > 0)
    def _():
        greet({"tm": slot, "space": rank - 1})

    @pl.when(rank < space_size - 1)
    def _():
        greet({"tm": slot, "space": rank + 1})

    greet(at_slot(before))

    @pl.when(fine)
    def _():
        greet(at_slot(above))

        @pl.when(place == 0)
        def _():
            greet(at_slot(slot + tm_size - RING + 1))

    member, group = lax.rem(slot, GROUP), slot // GROUP
    groups = tm_size // GROUP
    def in_group(index):
        return at_slot(group * GROUP + index)

    def facing(index):
        return at_slot(index * GROUP + member)

    @pl.when(coarse)
    def _():
        def call(index, carry):
            greet(in_group(index))
            return carry

        lax.fori_loop(member + 1, GROUP, call, 0)

        def call_later(index, carry):
            greet(facing(index))
            return carry

        lax.fori_loop(group + 1, groups, call_later, 0)

    def begin_load(index, carry):
        for copy in loads(tile_at(index)):
            copy.start()
        return carry

    lax.fori_loop(0, TILES, begin_load, 0)
    mixed[:, :, pl.ds(8, 8), :] = jnp.zeros((TILES, 2, 8, LANES), F32)
    mixed[:, :, pl.ds(144, 8), :] = jnp.zeros((TILES, 2, 8, LANES), F32)

    with jax.named_scope("load"):
        for tile in range(FIRST_COARSE_TILE, FIRST_COARSE_TILE + COARSE_TILES):
            wait_load(tile)

    def count(flag):
        return flag.astype(jnp.int32)

    with jax.named_scope("barrier"):
        own_kind = jnp.where(coarse, member + group, 1 + count(place == 1))
        pl.semaphore_wait(barrier, 1 + count(rank > 0) + count(rank < space_size - 1) + own_kind)

    @pl.when(coarse)
    def _():
        def answer_earlier(index, carry):
            pl.semaphore_signal(ready_carry, inc=1, device_id=facing(index), device_id_type=MESH)
            return carry

        lax.fori_loop(0, group, answer_earlier, 0)

        def answer(index, carry):
            pl.semaphore_signal(ready, inc=1, device_id=in_group(index), device_id_type=MESH)
            return carry

        lax.fori_loop(0, member, answer, 0)

    parts = (pl.ds(FIRST_COARSE_TILE, COARSE_TILES), pl.ds(0, FIRST_COARSE_TILE),
             pl.ds(FIRST_COARSE_TILE + COARSE_TILES, TILES - FIRST_COARSE_TILE - COARSE_TILES))

    def halo(side, part):
        low, high = (ROWS, 0) if side == 0 else (8, ROWS + 8)
        return pltpu.make_async_remote_copy(
            src_ref=fields.at[parts[part], :, pl.ds(low, 8), :], dst_ref=fields.at[parts[part], :, pl.ds(high, 8), :],
            send_sem=halo_send.at[side], recv_sem=halo_recv.at[side, part],
            device_id={"tm": slot, "space": rank + 1 if side == 0 else rank - 1}, device_id_type=MESH)

    def send_halo(*which):
        @pl.when(rank < space_size - 1)
        def _():
            for part in which:
                halo(0, part).start()

        @pl.when(rank > 0)
        def _():
            for part in which:
                halo(1, part).start()

    def wait_halo(*which):
        @pl.when(rank > 0)
        def _():
            for part in which:
                halo(0, part).wait_recv()

        @pl.when(rank < space_size - 1)
        def _():
            for part in which:
                halo(1, part).wait_recv()

    def all_of(ref, send, recv):
        return pltpu.make_async_remote_copy(
            src_ref=ref, dst_ref=ref, send_sem=send, recv_sem=recv, device_id=at_slot(after), device_id_type=MESH)

    def halo_sent():
        edge_rows = fields.at[:, :, pl.ds(0, 8), :]

        @pl.when(rank < space_size - 1)
        def _():
            all_of(edge_rows, halo_send.at[0], halo_recv.at[0, 0]).wait_send()

        @pl.when(rank > 0)
        def _():
            all_of(edge_rows, halo_send.at[1], halo_recv.at[0, 0]).wait_send()

    send_halo(0)

    def bulk(rows, cols, index=0):
        return pltpu.make_async_remote_copy(
            src_ref=nodes_out.at[pl.ds(2, 2), rows, cols], dst_ref=next_out.at[:, rows, cols],
            send_sem=bulk_send.at[index], recv_sem=bulk_recv, device_id=at_slot(after), device_id_type=MESH)

    def push(rows, cols, index=0):
        @pl.when(slot < tm_size - 1)
        def _():
            bulk(rows, cols, index).start()

    def field(tile, plane, low, high):
        return fields[tile, plane, pl.ds(low + 8, high - low), :]

    def mix(tile, low, high):
        for part in range(2):
            mixed[tile, part, pl.ds(low + 16, high - low), :] = (
                (5.0 / 24.0) * field(tile, part, low, high) + (1.0 / 3.0) * field(tile, 2 + part, low, high)
                - (1.0 / 24.0) * field(tile, 4 + part, low, high))

    def beside(ref, lead, low, high):
        count = high - low
        real = ref[(*lead, 0, pl.ds(low + 15, count), slice(None))] + ref[(*lead, 0, pl.ds(low + 17, count), slice(None))]
        imag = ref[(*lead, 1, pl.ds(low + 15, count), slice(None))] + ref[(*lead, 1, pl.ds(low + 17, count), slice(None))]
        return real, imag

    def rates(tile, low, high):
        return rate_of(rank * ROWS + low, tile * LANES, high - low)

    def one(tile, low, high, scale=None, keep=False):
        rate_real, rate_imag, factor = rates(tile, low, high)
        inv_real, inv_imag = inverse(1.0 - 0.5 * rate_real, -0.5 * rate_imag)
        sum_real, sum_imag = beside(mixed, (tile,), low, high)
        begin = [field(tile, part, low, high) for part in range(2)]
        old_one = [field(tile, 2 + part, low, high) for part in range(2)]
        old_two = [field(tile, 4 + part, low, high) for part in range(2)]
        own = [(5.0 / 24.0) * begin[i] - (1.0 / 6.0) * old_one[i] - (1.0 / 24.0) * old_two[i] for i in range(2)]
        top = times(rate_real, rate_imag, *own)
        node = times(inv_real, inv_imag, begin[0] + top[0] + factor * sum_imag, begin[1] + top[1] - factor * sum_real)
        if scale is not None:
            node = [part * scale for part in node]
        for i in range(2):
            staged[tile, i, pl.ds(low + 16, high - low), :] = (
                (5.0 / 24.0) * old_two[i] - (1.0 / 24.0) * begin[i] - (1.0 / 6.0) * old_one[i] + 0.5 * node[i])
            if keep:
                node_one_buf[i, pl.ds(low + 16, high - low), :] = node[i]
            first, last = max(low, 0), min(high, ROWS)
            if first < last:
                nodes_out[i, pl.ds(first, last - first), columns(tile)] = node[i][first - low:last - low]

    def two(tile, low, high, keep=False):
        rate_real, rate_imag, factor = rates(tile, low, high)
        inv_real, inv_imag = inverse(1.0 - 0.5 * rate_real, -0.5 * rate_imag)
        sum_real, sum_imag = beside(staged, (tile,), low, high)
        begin = [field(tile, part, low, high) for part in range(2)]
        old_one = [field(tile, 2 + part, low, high) for part in range(2)]
        old_two = [field(tile, 4 + part, low, high) for part in range(2)]
        if keep:
            node = [node_one_buf[i, pl.ds(low + 16, high - low), :] for i in range(2)]
        else:
            node = [nodes_out[i, pl.ds(low, high - low), columns(tile)] for i in range(2)]
        own = [(1.0 / 3.0) * old_one[i] - (1.0 / 24.0) * begin[i] - (7.0 / 24.0) * old_two[i] for i in range(2)]
        top = times(rate_real, rate_imag, *own)
        last_node = times(inv_real, inv_imag, node[0] + top[0] + factor * sum_imag, node[1] + top[1] - factor * sum_real)
        for i in range(2):
            if keep:
                whole[i, pl.ds(low + 16, high - low), :] = (
                    (1.0 / 6.0) * begin[i] + (2.0 / 3.0) * node[i] + (1.0 / 6.0) * last_node[i])
            first, last = max(low, 0), min(high, ROWS)
            if first < last:
                nodes_out[2 + i, pl.ds(first, last - first), columns(tile)] = last_node[i][first - low:last - low]

    def inner(tile):
        for low in range(0, ROWS, 32):
            mix(tile, low, low + 32)
        for low in range(0, ROWS, 32):
            one(tile, low, low + 32)
        for low in (8, 40, 72, 104):
            two(tile, low, min(low + 32, 120))

    def rim(tile):
        mix(tile, -8, 0)
        mix(tile, ROWS, ROWS + 8)
        one(tile, -8, 8, scale=jnp.concatenate([jnp.full((8, LANES), (rank > 0).astype(F32)), jnp.ones((8, LANES), F32)]))
        one(tile, 120, 136,
            scale=jnp.concatenate([jnp.ones((8, LANES), F32), jnp.full((8, LANES), (rank < space_size - 1).astype(F32))]))
        two(tile, 0, 8)
        two(tile, 120, 128)

    middle = pl.ds(8, 112)
    upper = pl.ds(0, 8)
    lower = pl.ds(120, 8)

    def edge(index, carry):
        rim(tile_at(index))
        return carry

    def settle(cols):
        @pl.when(slot > 0)
        def _():
            bulk(slice(None), cols).wait_recv()

    @pl.when(fine)
    def _():
        def relay_source(chunk):
            rows = pl.ds(pl.multiple_of(8 + lax.rem(chunk, 2) * RELAY_ROWS, 8), RELAY_ROWS)
            return rows, columns(tile_at(LEAD + chunk // 2))

        def leg(which, chunk):
            rows, cols = relay_source(chunk)
            if which == 0:
                source, target, device = nodes_out.at[pl.ds(2, 2), rows, cols], first_leg.at[chunk], at_slot(below)
                recv = relay_recv.at[0, chunk]
            elif which == 1:
                source, target, device, recv = first_leg.at[chunk], second_leg.at[chunk], at_slot(below), relay_recv.at[1, chunk]
            else:
                origin = column * RING + lax.rem(place + 2, RING)
                source, target, device, recv = second_leg.at[chunk], next_out.at[:, rows, cols], at_slot(origin + 1), bulk_recv
            return pltpu.make_async_remote_copy(
                src_ref=source, dst_ref=target, send_sem=relay_send.at[which], recv_sem=recv,
                device_id=device, device_id_type=MESH)

        def relayed(which):
            start = lax.rem(place + which, RING)
            wraps = (start == RING - 1).astype(jnp.int32)
            return 4 + RELAY_WRAP * wraps + count(shared) * (RELAY_SHARED + RELAY_BOTH * wraps)

        def has_origin(which):
            return column * RING + lax.rem(place + which, RING) < tm_size - 1

        def start_tile(index, carry):
            @pl.when(index >= COARSE_TILES)
            def _():
                wait_load(tile_at(index))

            inner(tile_at(index))
            first = 2 * (index - LEAD)
            chunks = jnp.where(first < 0, 0, relayed(0) - first)

            @pl.when(has_origin(0) & (chunks > 0))
            def _():
                leg(0, first).start()

            @pl.when(has_origin(0) & (chunks > 1))
            def _():
                leg(0, first + 1).start()

            @pl.when(has_origin(0) & (chunks == 1))
            def _():
                bulk(pl.ds(8 + RELAY_ROWS, RELAY_ROWS), columns(tile_at(index))).start()

            @pl.when(has_origin(0) & (chunks <= 0))
            def _():
                bulk(middle, columns(tile_at(index))).start()

            return carry

        def forward(which, chunk):
            @pl.when(has_origin(which) & (chunk >= 0) & (chunk < relayed(which)))
            def _():
                leg(which - 1, chunk).wait_recv()
                leg(which, chunk).start()

        with jax.named_scope("inner"):
            lax.fori_loop(0, TILES, start_tile, 0)
        send_halo(1, 2)
        with jax.named_scope("fwdA"):
            forward(1, 0)
            forward(1, 1)
        with jax.named_scope("halo"):
            wait_halo(0, 1, 2)

        @pl.when(rank == 0)
        def _():
            fields[:, :, pl.ds(0, 8), :] = jnp.zeros((TILES, 6, 8, LANES), F32)

        @pl.when(rank == space_size - 1)
        def _():
            fields[:, :, pl.ds(ROWS + 8, 8), :] = jnp.zeros((TILES, 6, 8, LANES), F32)

        with jax.named_scope("rim"):
            lax.fori_loop(0, TILES, edge, 0)
        push(upper, slice(None), 1)
        push(lower, slice(None), 1)

        def pass_on(step, carry):
            forward(1, step)
            forward(2, step - LAG)
            return carry

        with jax.named_scope("fwdB"):
            lax.fori_loop(2, RELAYS + LAG, pass_on, 0)
        halo_sent()

        for relays in range(4, RELAYS + 1):
            chunks = first_leg.at[pl.ds(0, relays)]
            direct = fields.at[pl.ds(0, 7), pl.ds(0, 2), pl.ds(0, 8 * (2 * TILES - relays)), :]
            for which in range(3):
                @pl.when(has_origin(which) & (relayed(which) == relays))
                def _():
                    all_of(chunks, relay_send.at[which], relay_recv.at[0, 0]).wait_send()

            @pl.when(has_origin(0) & (relayed(0) == relays))
            def _():
                all_of(direct, bulk_send.at[0], relay_recv.at[0, 0]).wait_send()

        @pl.when(has_origin(0))
        def _():
            bulk(pl.ds(0, 16), slice(None), 1).wait_send()

        with jax.named_scope("settle"):
            settle(slice(None))

    @pl.when(coarse)
    def _():
        lead = (slot == 0).astype(F32)

        def piece(index):
            share = GROUP // COARSE_TILES
            rows = pl.ds(pl.multiple_of(lax.rem(index, share) * PIECE_ROWS, 8), PIECE_ROWS)
            return index // share, slice(None), rows, slice(None)

        def push_only(index, carry):
            push(middle, columns(tile_at(index)))
            return carry

        lax.fori_loop(COARSE_TILES, TILES, lambda index, carry: (wait_load(tile_at(index)), carry)[1], 0)
        send_halo(1, 2)
        with jax.named_scope("innerA"):
            def inner_and_push(index, carry):
                inner(tile_at(index))

                @pl.when(index < first_pushes)
                def _():
                    push_only(index, 0)

                return carry

            first_pushes = COARSE_TILES + jnp.where(place == RING - 1, FIRST_WRAP + LAST_FIRST * count(group == groups - 1), FIRST)
            lax.fori_loop(COARSE_TILES, TILES, inner_and_push, 0)
        with jax.named_scope("halo"):
            wait_halo(0)

        def full(tile, carry):
            bands = ((-8, 24), (24, 56), (56, 88), (88, 120), (120, 136))
            for low, high in bands:
                mix(tile, low, high)
            for low, high in bands:
                one(tile, low, high, keep=True)
            for low, high in bands:
                two(tile, low, high, keep=True)
            for low in range(0, ROWS, 32):
                rate_real, rate_imag, factor = rates(tile, low, low + 32)
                sum_real, sum_imag = beside(whole, (), low, low + 32)
                own = [whole[i, pl.ds(low + 16, 32), :] - nodes_out[2 + i, pl.ds(low, 32), columns(tile)] for i in range(2)]
                top = times(rate_real, rate_imag, *own)
                offset[tile - FIRST_COARSE_TILE, 0, pl.ds(low, 32), :] = top[0] + factor * sum_imag + lead * field(tile, 0, low, low + 32)
                offset[tile - FIRST_COARSE_TILE, 1, pl.ds(low, 32), :] = top[1] - factor * sum_real + lead * field(tile, 1, low, low + 32)
            return carry

        def gather(source, target):
            return pltpu.make_async_remote_copy(
                src_ref=offset.at[piece(target)], dst_ref=gathered.at[source], send_sem=gather_send,
                recv_sem=gather_recv, device_id=in_group(target), device_id_type=MESH)

        def scatter(source, target):
            return pltpu.make_async_remote_copy(
                src_ref=results.at[target], dst_ref=begins.at[piece(source)], send_sem=scatter_send,
                recv_sem=scatter_recv, device_id=in_group(target), device_id_type=MESH)

        def hand_on(source, target):
            return pltpu.make_async_remote_copy(
                src_ref=carry_out, dst_ref=carry_in.at[source], send_sem=carry_send,
                recv_sem=carry_recv, device_id=facing(target), device_id_type=MESH)

        row = member // RING
        beside_row = (row + 1 - 2 * lax.rem(row, 2)) * RING

        def detour(stage):
            source = offset.at[piece(row * RING)] if stage == 0 else results.at[row * RING]
            sem = gather_send if stage == 0 else scatter_send
            return pltpu.make_async_remote_copy(
                src_ref=source, dst_ref=aside.at[stage], send_sem=sem, recv_sem=aside_recv.at[stage],
                device_id=in_group(beside_row), device_id_type=MESH)

        def relay_aside(stage):
            origin = beside_row + RING - 1
            target = gathered.at[origin] if stage == 0 else begins.at[piece(origin)]
            sem = gather_recv if stage == 0 else scatter_recv
            return pltpu.make_async_remote_copy(
                src_ref=aside.at[stage], dst_ref=target, send_sem=aside_send.at[stage], recv_sem=sem,
                device_id=in_group(beside_row), device_id_type=MESH)

        def crowded(stage, row):
            return (group > 0) & (row == 0) if stage == 0 else (group == 0) & (row == 1)

        def pass_aside(stage):
            @pl.when((place == 0) & crowded(stage, 1 - row))
            def _():
                detour(stage).wait_recv()
                relay_aside(stage).start()

        def blocked(target, stage):
            return (place == RING - 1) & (target == row * RING) & crowded(stage, row)

        others = gathered.at[pl.ds(0, GROUP - 1)]

        def other(distance):
            return lax.rem(member + distance, GROUP)

        with jax.named_scope("full"):
            lax.fori_loop(FIRST_COARSE_TILE, FIRST_COARSE_TILE + COARSE_TILES, full, 0)
        with jax.named_scope("ready"):
            @pl.when(member < GROUP - 1)
            def _():
                pl.semaphore_wait(ready, GROUP - 1 - member)

        def spread(distance, carry):
            @pl.when(jnp.logical_not(blocked(other(distance), 0)))
            def _():
                gather(member, other(distance)).start()

            return carry

        with jax.named_scope("spread"):
            @pl.when((place == RING - 1) & crowded(0, row))
            def _():
                detour(0).start()

            lax.fori_loop(1, GROUP, spread, 0)
        gathered[member] = offset[piece(member)]
        early = jnp.where(place == RING - 1, EARLY_WRAP + group * WRAP_STEP // 2, EARLY + count(place == 0) * EARLY_ZERO + group * EARLY_STEP // 2)
        early = jnp.minimum(early + LAST_WRAP * count((place == RING - 1) & (group == groups - 1)), TILES)
        early = jnp.maximum(early, first_pushes)
        lax.fori_loop(first_pushes, early, push_only, 0)
        with jax.named_scope("halo2"):
            wait_halo(1, 2)
        with jax.named_scope("rim"):
            lax.fori_loop(COARSE_TILES, TILES, edge, 0)
        left = pl.ds(0, FIRST_COARSE_TILE * LANES)
        right_start = (FIRST_COARSE_TILE + COARSE_TILES) * LANES
        right = pl.ds(right_start, KY - right_start)
        rims = [(upper, left), (upper, right), (lower, left), (lower, right)]
        for rows, cols in rims:
            push(rows, cols, 1)
        tile, _, _, _ = piece(member)
        first = lax.rem(member, GROUP // COARSE_TILES) * PIECE_ROWS
        rate_real, rate_imag, _ = rate_of(rank * ROWS + first, (FIRST_COARSE_TILE + tile) * LANES, PIECE_ROWS)
        gain = inverse(1.0 - rate_real, -rate_imag)

        with jax.named_scope("aside0"):
            pass_aside(0)
        with jax.named_scope("gather"):
            all_of(others, gather_send, gather_recv).wait_recv()

        def scan(index, running):
            for i in range(2):
                prefix[index, i] = running[i]
            return times(*gain, running[0] + gathered[index, 0], running[1] + gathered[index, 1])

        nothing = jnp.zeros((PIECE_ROWS, LANES), F32)
        with jax.named_scope("scan"):
            running = lax.fori_loop(0, GROUP, scan, (nothing, nothing))
            for i in range(2):
                carry_out[i] = running[i]

            @pl.when(group < groups - 1)
            def _():
                pl.semaphore_wait(ready_carry, groups - 1 - group)

            def tell(target, carry):
                hand_on(group, target).start()
                return carry

            lax.fori_loop(group + 1, groups, tell, 0)

        jump = gain
        for _ in range(GROUP.bit_length() - 1):
            jump = times(*jump, *jump)

        def join(source, running):
            far = times(*jump, *running)
            return far[0] + carry_in[source, 0], far[1] + carry_in[source, 1]

        with jax.named_scope("carry"):
            for number in range(1, groups):
                @pl.when(group == number)
                def _():
                    all_of(carry_in.at[pl.ds(0, number)], carry_send, carry_recv).wait_recv()

            entering = lax.fori_loop(0, group, join, (nothing, nothing))

        def add_carry(index, running):
            for i in range(2):
                results[index, i] = prefix[index, i] + running[i]
            return times(*gain, *running)

        lax.fori_loop(0, GROUP, add_carry, entering)

        def give(distance, carry):
            @pl.when(jnp.logical_not(blocked(other(distance), 1)))
            def _():
                scatter(member, other(distance)).start()

            return carry

        with jax.named_scope("give"):
            @pl.when((place == RING - 1) & crowded(1, row))
            def _():
                detour(1).start()

            lax.fori_loop(1, GROUP, give, 0)
        begins[piece(member)] = results[member]
        lax.fori_loop(early, TILES, push_only, 0)

        with jax.named_scope("aside1"):
            pass_aside(1)
        with jax.named_scope("back"):
            all_of(others, scatter_send, scatter_recv).wait_recv()

        later = 1.0 - lead

        def finish(tile, carry):
            which = tile - FIRST_COARSE_TILE
            for low in range(0, ROWS, 32):
                rows = pl.ds(low, 32)
                rate_real, rate_imag, _ = rates(tile, low, low + 32)
                inv_real, inv_imag = inverse(1.0 - rate_real, -rate_imag)
                begin_new = [begins[which, i, rows, :] for i in range(2)]
                end_new = times(inv_real, inv_imag, *[begin_new[i] + offset[which, i, rows, :] for i in range(2)])
                for i in range(2):
                    old_end = nodes_out[2 + i, rows, columns(tile)]
                    nodes_out[i, rows, columns(tile)] += 0.5 * (
                        (begin_new[i] - later * field(tile, i, low, low + 32)) + (end_new[i] - old_end))
                    nodes_out[2 + i, rows, columns(tile)] = end_new[i]
                    next_out[i, rows, columns(tile)] = begin_new[i]
            return carry

        with jax.named_scope("finish"):
            lax.fori_loop(FIRST_COARSE_TILE, FIRST_COARSE_TILE + COARSE_TILES, finish, 0)

        halo_sent()

        for number in range(1, groups):
            @pl.when(group == groups - 1 - number)
            def _():
                all_of(carry_in.at[pl.ds(0, number)], carry_send, carry_recv).wait_send()

        all_of(others, gather_send, gather_recv).wait_send()
        all_of(others, scatter_send, scatter_recv).wait_send()

        for stage in range(2):
            @pl.when((place == 0) & crowded(stage, 1 - row))
            def _():
                relay_aside(stage).wait_send()

        @pl.when(slot < tm_size - 1)
        def _():
            bulk(middle, pl.ds(0, FINE_TILES * LANES)).wait_send()
            bulk(pl.ds(0, 16), pl.ds(0, FINE_TILES * LANES), 1).wait_send()

        with jax.named_scope("settle"):
            settle(pl.ds(0, FINE_TILES * LANES))

    @pl.when(slot == 0)
    def _():
        def restore(tile, carry):
            for i in range(2):
                next_out[i, :, columns(tile)] = fields[tile, i, pl.ds(8, ROWS), :]
            return carry

        lax.fori_loop(0, TILES, restore, 0)


def deliver(start_ref, nodes_ref, start_hbm, nodes_hbm, sem):
    def copies(source, target, planes):
        return [pltpu.make_async_copy(source.at[i, pl.ds(row, DELIVER_ROWS)], target.at[i, pl.ds(row, DELIVER_ROWS)], sem)
                for i in range(planes) for row in range(0, ROWS, DELIVER_ROWS)]

    for copy in copies(nodes_ref, nodes_hbm, 4) + copies(start_ref, start_hbm, 2):
        copy.start()
    pltpu.make_async_copy(nodes_ref, nodes_hbm, sem).wait()
    pltpu.make_async_copy(start_ref, start_hbm, sem).wait()


def solution(mesh):
    tm_size, space_size = mesh.shape["tm"], mesh.shape["space"]

    def body(start_values, node_values):
        hbm = pl.BlockSpec(memory_space=pltpu.MemorySpace.HBM)
        vmem = pl.BlockSpec(memory_space=pltpu.MemorySpace.VMEM)
        dma = pltpu.SemaphoreType.DMA
        next_start, nodes = pl.pallas_call(
            functools.partial(kernel, tm_size, space_size),
            out_shape=(pltpu.MemorySpace.VMEM((2, ROWS, KY), F32), pltpu.MemorySpace.VMEM((4, ROWS, KY), F32)),
            in_specs=[hbm, hbm],
            out_specs=(vmem, vmem),
            scratch_shapes=[
                pltpu.VMEM((TILES, 6, ROWS + 16, LANES), F32),
                pltpu.VMEM((TILES, 2, ROWS + 32, LANES), F32),
                pltpu.VMEM((TILES, 2, ROWS + 32, LANES), F32),
                pltpu.VMEM((2, ROWS + 32, LANES), F32),
                pltpu.VMEM((2, ROWS + 32, LANES), F32),
                pltpu.VMEM((COARSE_TILES, 2, ROWS, LANES), F32),
                pltpu.VMEM((GROUP, 2, PIECE_ROWS, LANES), F32),
                pltpu.VMEM((GROUP, 2, PIECE_ROWS, LANES), F32),
                pltpu.VMEM((tm_size // GROUP, 2, PIECE_ROWS, LANES), F32),
                pltpu.VMEM((2, PIECE_ROWS, LANES), F32),
                pltpu.VMEM((GROUP, 2, PIECE_ROWS, LANES), F32),
                pltpu.VMEM((COARSE_TILES, 2, ROWS, LANES), F32),
                pltpu.VMEM((RELAYS, 2, RELAY_ROWS, LANES), F32),
                pltpu.VMEM((RELAYS, 2, RELAY_ROWS, LANES), F32),
                dma((TILES,)),
                dma((2,)),
                dma((2, 3)),
                dma((2,)),
                dma,
                dma,
                dma,
                dma,
                dma,
                dma,
                dma,
                dma((3,)),
                dma((2, RELAYS)),
                pltpu.SemaphoreType.REGULAR,
                pltpu.SemaphoreType.REGULAR,
                pltpu.VMEM((2, 2, PIECE_ROWS, LANES), F32),
                dma((2,)),
                dma((2,)),
            ],
            compiler_params=pltpu.CompilerParams(collective_id=0, has_side_effects=True, vmem_limit_bytes=61696 * 1024),
            name="pfasst",
        )(start_values[0], node_values[0].reshape(4, ROWS, KY))
        next_start, nodes = pl.pallas_call(
            deliver,
            out_shape=(jax.ShapeDtypeStruct((2, ROWS, KY), F32), jax.ShapeDtypeStruct((4, ROWS, KY), F32)),
            in_specs=[vmem, vmem],
            out_specs=(hbm, hbm),
            scratch_shapes=[dma],
            compiler_params=pltpu.CompilerParams(vmem_limit_bytes=2**20),
            name="deliver",
        )(next_start, nodes)
        return next_start[None], nodes.reshape(1, 2, 2, ROWS, KY)

    return jax.shard_map(
        body,
        mesh=mesh,
        in_specs=(P("tm", None, "space", None), P("tm", None, None, "space", None)),
        out_specs=(P("tm", None, "space", None), P("tm", None, None, "space", None)),
        check_vma=False,
    )
```
